256 devices in a mesh: groups: 2 (over y), grid: 32 (over z, core), depth: 4 (over x).
Axes of the slice: x: 4, y: 2, z: 16, core: 2. Of those that a mesh axis runs over, the one named last changes fastest.
The devices are a block of a 4x16x16 slice.
Arguments:
- tokens: bfloat16 [4096, 4096], P(('groups', 'grid'), 'depth'), parts along dimension 0, may hold values from -6 to 6
- gate_weight: bfloat16 [4096, 14336], P('depth', 'grid'), may hold values from -0.09375 to 0.09375
- up_weight: bfloat16 [4096, 14336], P('depth', 'grid'), may hold values from -0.09375 to 0.09375
- down_weight: bfloat16 [14336, 4096], P('grid', 'depth'), may hold values from -0.046875 to 0.046875
Outputs:
- mixed: bfloat16 [4096, 4096], P(('groups', 'grid'), 'depth'), parts along dimension 0
The draws below stay inside these ranges and needn't reach their ends.
There are 2 independent parts, one for each index of `groups`. The reference program is written for one: setup_inputs(seed, part) draws one part's arguments, and reference() takes and returns one part's arrays. A program takes and returns all parts, laid end to end along the dimension named above; an argument that names none is the same for every part. Nothing has to cross between parts.
All inputs are finite; a program needn't handle non-finite values.
Results may differ from the reference program's by a relative error of at most 0.0049.
Values may be sent and summed in bfloat16 or wider, within the bound.
A program may use at most 64 MiB of HBM per device.

```python
import jax
import jax.numpy as jnp

D = 4096
FF = 14336
TOK = 2048


def steps_of(rng, extent, pieces, low, largest):
    loudness, own = 1.0, jax.random.fold_in(rng, 6)
    for axis_at, shards_of in pieces:
        draws = jnp.exp(jax.random.uniform(jax.random.fold_in(own, axis_at), (shards_of,), jnp.float32, low / len(pieces), largest / len(pieces)))
        loudness = loudness * jnp.repeat(draws, extent[axis_at] // shards_of).reshape([-1 if axis == axis_at else 1 for axis in range(len(extent))])
    return loudness


def noise(stream_key, dims, spread, limit, split=(), kind=jnp.bfloat16):
    entries = jax.random.normal(stream_key, dims, jnp.float32) * spread
    if len(split) > 0:
        entries = steps_of(stream_key, dims, split, -0.22, 0.18) * entries
    return jnp.clip(entries, min=-limit, max=limit).astype(kind)


def setup_inputs(seed: int = 0, part: int = 0) -> dict:
    keys = jax.random.split(jax.random.key(seed), 5)
    own_keys = jax.random.split(jax.random.fold_in(keys[4], part), 5)
    return {
        "tokens": noise(own_keys[0], (TOK, D), 1.0, 6.0, ((0, 32), (1, 4))),
        "gate_weight": noise(keys[1], (D, FF), D ** -0.5, 0.09375, ((0, 4), (1, 32))),
        "up_weight": noise(keys[2], (D, FF), D ** -0.5, 0.09375, ((0, 4), (1, 32))),
        "down_weight": noise(keys[3], (FF, D), FF ** -0.5, 0.046875, ((0, 32), (1, 4))),
    }


def reference(tokens, gate_weight, up_weight, down_weight):
    gate = jnp.dot(tokens, gate_weight, preferred_element_type=jnp.float32)
    up = jnp.dot(tokens, up_weight, preferred_element_type=jnp.float32)
    hidden = (jax.nn.silu(gate) * up).astype(jnp.bfloat16)
    return jnp.dot(hidden, down_weight, preferred_element_type=jnp.float32).astype(jnp.bfloat16)
```

```python
import functools

import jax
import jax.numpy as jnp
from jax import lax
from jax.experimental import pallas as pl
from jax.experimental.pallas import tpu as pltpu
from jax.sharding import PartitionSpec as P

F32 = jnp.float32
BF16 = jnp.bfloat16

A_PIECES = 4
D_PIECES = 2
WIDE_HOPS = 3
LAG = 3


class Plan:
    def __init__(self, chips, block):
        self.S = chips // 2
        self.block = block
        self.total = block * chips

    def off(self, s):
        return 0 if s == 0 else self.block * (2 * s - 1)

    def rows(self, s):
        return self.block if s in (0, self.S) else 2 * self.block

    def order(self):
        half = self.S // 2
        return list(range(half)) + list(range(self.S, half - 1, -1))

    def pieces(self, s, way, n):
        if s < self.S:
            return list(range(n))
        return list(range(n // 2)) if way == 0 else list(range(n // 2, n))

    def ops(self):
        S, out = self.S, []
        za, zd = 2.8 / A_PIECES, 2.8 / D_PIECES
        out.append((("A", 0, 0), [], [], [(("a", 1, p), "z", za) for p in range(A_PIECES)], 0.1, 0))
        for s in range(1, S + 1):
            for p in range(A_PIECES):
                send = [(("a", s + 1, p), "z", za if s + 1 < S else za / 2)] if s < S else []
                out.append((("A", s, p), [("A", 0, 0)], [("a", s, p)], send, 0.06, 0))
        seq = self.order()
        for i, s in enumerate(seq):
            u = self.rows(s) / (2 * self.block)
            deps = [("A", s, p) for p in range(A_PIECES)] if s else [("A", 0, 0)]
            if i:
                deps.append(("M", seq[i - 1]))
            if i >= LAG:
                deps.append(("S", seq[i - LAG]))
            x = 1.23 * u
            out.append((("M", s), deps, [], [(("r", s), "x", x), (("d", s), "x", x)], 0.4 + 1.2 * u, 6))
            out.append((("R", s), [("M", s)], [("r", s)], [(("e", s), "x", x)], 0.15, 1))
            out.append((("S", s), [("R", s)], [("d", s), ("e", s)], [(("h", s), "x", x)], 0.3, 2))
            out.append((("F", s), [("S", s)], [("h", s)], [(("f", s), "x", x / 2)], 0.05, 1))
            out.append((("N", s), [("F", s)], [("f", s)], [], 0.3 + 0.5 * u, 5))
        for s in range(S, -1, -1):
            for p in range(D_PIECES):
                deps = [("N", s)]
                if s < S:
                    deps += [("Z", s + 1, q) for q in range(D_PIECES)]
                wait = [("z", s, p)] if s < S else []
                wide = 2 if s <= WIDE_HOPS else 1
                send = [(("z", s - 1, p), "z", wide * (zd if s < S else zd / 2))] if s else []
                out.append((("Z", s, p), deps, wait, send, 0.15, 4))
        return out

    def schedule(self, latency=2.2, start=3.5):
        ops = self.ops()
        done, arrives, free = set(), {}, {"x": 0.0, "z": 0.0}
        now, result = 0.0, []
        while ops:
            best = None
            for k, (name, deps, wait, send, cost, rank) in enumerate(ops):
                if any(d not in done for d in deps) or any(m not in arrives for m in wait):
                    continue
                ready = max([now] + [arrives[m] for m in wait])
                if name[0] == "M":
                    ready = max(ready, start)
                key = (ready, rank, k)
                if best is None or key < best[0]:
                    best = (key, k)
            name, deps, wait, send, cost, rank = ops.pop(best[1])
            now = best[0][0] + cost
            for message, link, length in send:
                free[link] = max(free[link], now) + length
                arrives[message] = free[link] + latency
            done.add(name)
            result.append((name, round(now, 2)))
        return result


def kernel(plan, tok, wg, wu, wd, out, X, W, WD, GV, UV, PB, SR, RR, SD, RD, H, O, ZS, ZR, YS, YR,
           local_sem, send_sem, recv_sem):
    S, B = plan.S, plan.block
    ring = 2 * 2 * S
    width = wg.shape[1]
    grid, me = lax.axis_index("grid"), lax.axis_index("depth")
    core = lax.rem(grid, 2)
    other = 1 - core
    partner = {"grid": grid + 1 - 2 * core}
    zway = ({"grid": lax.rem(grid + 2, ring)}, {"grid": lax.rem(grid + ring - 2, ring)})
    xway = ({"depth": lax.rem(me + 1, 4)}, {"depth": lax.rem(me + 3, 4)})

    numbers, started = {}, []

    def message(key, src, dst, to):
        n = numbers.setdefault(key, len(numbers))
        return pltpu.make_async_remote_copy(
            src_ref=src, dst_ref=dst, send_sem=send_sem.at[n], recv_sem=recv_sem.at[n],
            device_id=to, device_id_type=pl.DeviceIdType.MESH)

    def send(key, src, dst, to):
        m = message(key, src, dst, to)
        m.start()
        started.append(m)

    def arrived(key, dst, to):
        message(key, dst, dst, to).wait_recv()

    loads = [
        pltpu.make_async_copy(tok, X.at[pl.ds(0, B)], local_sem.at[0]),
        pltpu.make_async_copy(wg, GV, local_sem.at[1]),
        pltpu.make_async_copy(wu, UV, local_sem.at[2]),
        pltpu.make_async_copy(wd, WD.at[core], local_sem.at[3]),
    ]
    for load in loads:
        load.start()

    barrier = pltpu.get_barrier_semaphore()
    for to in (*zway, *xway, partner):
        pl.semaphore_signal(barrier, inc=1, device_id=to, device_id_type=pl.DeviceIdType.MESH)
    pl.semaphore_wait(barrier, 5)

    def a_rows(s, way, p):
        size = B // A_PIECES
        base = plan.off(s) + (B if way == 1 and 0 < s < S else 0)
        return pl.ds(base + p * size, size)

    def a_send(s, p):
        for way in (0, 1):
            if p in plan.pieces(s + 1, way, A_PIECES):
                send(("a", s + 1, way, p), X.at[a_rows(s, way, p)], X.at[a_rows(s + 1, way, p)], zway[way])

    def op_a(s, p=None):
        if s == 0:
            loads[0].wait()
            for p in range(A_PIECES):
                a_send(0, p)
            for load in loads[1:3]:
                load.wait()

            @pl.loop(0, wg.shape[0] // 128)
            def _(i):
                r = pl.ds(pl.multiple_of(i * 128, 128), 128)
                W[core, r, :] = jnp.concatenate([GV[r, :], UV[r, :]], axis=1)

            send(("w",), W.at[core], W.at[core], partner)
            loads[3].wait()
            send(("v",), WD.at[core], WD.at[core], partner)
            return
        for way in (0, 1):
            if p in plan.pieces(s, way, A_PIECES):
                dst = X.at[a_rows(s, way, p)]
                arrived(("a", s, way, p), dst, zway[way])
        if s < S:
            a_send(s, p)

    def quarter(s, k):
        size = plan.rows(s) // 4
        return pl.ds(pl.multiple_of(plan.off(s) + lax.rem(me + k, 4) * size, 16), size)

    def packed(s):
        return pl.ds(plan.off(s) // 4, plan.rows(s) // 4)

    def op_m(s):
        if s == 0:
            arrived(("w",), W.at[other], partner)
        r, q = pl.ds(plan.off(s), plan.rows(s)), packed(s)
        for half in (0, 1):
            PB[half, r, :] = jnp.dot(X[r, :], W[half], preferred_element_type=F32)
            SR[half, q, :] = PB[half, quarter(s, 2), :].astype(BF16)
            send(("r", s, half), SR.at[half, q], RR.at[half, q], xway[half])
        for way in (0, 1):
            half = 1 - way
            SD[way, half, q, :] = PB[half, quarter(s, 1 + 2 * way), :].astype(BF16)
            send(("d", s, way, half), SD.at[way, half, q], RD.at[way, half, q], xway[way])

    def op_r(s):
        q = packed(s)
        for way in (0, 1):
            arrived(("r", s, way), RR.at[way, q], xway[way])
            SD[way, way, q, :] = (PB[way, quarter(s, 1 + 2 * way), :] + RR[way, q, :].astype(F32)).astype(BF16)
            send(("d", s, way, way), SD.at[way, way, q], RD.at[way, way, q], xway[way])

    def op_s(s):
        q, mine = packed(s), quarter(s, 0)
        parts = []
        for way in (0, 1):
            for half in (0, 1):
                arrived(("d", s, way, half), RD.at[way, half, q], xway[way])
        for half in (0, 1):
            t = PB[half, mine, :] + RD[0, half, q, :].astype(F32) + RD[1, half, q, :].astype(F32)
            gate, up = t[:, :width], t[:, width:]
            parts.append(gate / (1.0 + jnp.exp(-gate)) * up)
        H[mine, :] = jnp.concatenate(parts, axis=1).astype(BF16)
        for way in (0, 1):
            send(("h", s, way), H.at[mine], H.at[mine], xway[way])

    def passed_on(s, way, k):
        size = plan.rows(s) // 4
        if s in (0, S):
            return quarter(s, k) if way == (0 if s == 0 else 1) else None
        start = plan.off(s) + lax.rem(me + k, 4) * size + way * (size // 2)
        return pl.ds(pl.multiple_of(start, 16), size // 2)

    def op_f(s):
        for way in (0, 1):
            k = 3 - 2 * way
            arrived(("h", s, way), H.at[quarter(s, k)], xway[way])
            part = passed_on(s, way, k)
            if part is not None:
                send(("f", s, way), H.at[part], H.at[part], xway[way])

    def op_n(s):
        if s == plan.order()[0]:
            arrived(("v",), WD.at[other], partner)
        for way in (0, 1):
            part = passed_on(s, way, 2)
            if part is not None:
                arrived(("f", s, way), H.at[part], xway[way])
        r = pl.ds(plan.off(s), plan.rows(s))
        depth = WD.shape[0] * WD.shape[1]
        O[r, :] = jnp.dot(H[r, :], WD[...].reshape(depth, WD.shape[2]), preferred_element_type=F32)

    def z_place(s, way, p):
        size = B // D_PIECES
        r = pl.ds(s * B + p * size, size)
        return (YS.at[way, r], YR.at[way, r]) if s < WIDE_HOPS else (ZS.at[way, r], ZR.at[way, r])

    def op_z(s, p):
        size = B // D_PIECES
        total = None
        for way in (0, 1):
            if p not in plan.pieces(s, way, D_PIECES):
                continue
            if s == 0:
                base = 0
            else:
                base = plan.off(s) + (B if way == 0 and s < S else 0)
            if total is None or s > 0:
                total = O[pl.ds(base + p * size, size), :]
            if s < S and p in plan.pieces(s + 1, way, D_PIECES):
                got = z_place(s, way, p)[1]
                arrived(("z", s, way, p), got, zway[way])
                total = total + got[...].astype(F32)
            if s > 0:
                src, dst = z_place(s - 1, way, p)
                src[...] = total.astype(src.dtype)
                send(("z", s - 1, way, p), src, dst, zway[way])
        if s == 0:
            out[pl.ds(p * size, size), :] = total.astype(BF16)

    run = {"A": op_a, "M": op_m, "R": op_r, "S": op_s, "F": op_f, "N": op_n, "Z": op_z}
    for (name, *at), _ in plan.schedule():
        run[name](*at)
    for m in started:
        m.wait_send()


def messages(plan):
    S = plan.S
    a = 2 * ((S - 1) * A_PIECES + A_PIECES // 2)
    z = 2 * ((S - 1) * D_PIECES + D_PIECES // 2)
    return a + z + 2 + (S + 1) * 8 + 2 * (S - 1) + 2


def body(tokens, gate_weight, up_weight, down_weight):
    block, deep = tokens.shape
    width, cols = down_weight.shape
    chips = lax.axis_size("grid") // 2
    plan = Plan(chips, block)
    total, quarters = plan.total, plan.total // 4
    vmem, any_ = pl.BlockSpec(memory_space=pltpu.VMEM), pl.BlockSpec(memory_space=pl.ANY)
    n = messages(plan)
    return pl.pallas_call(
        functools.partial(kernel, plan),
        out_shape=jax.ShapeDtypeStruct((block, cols), BF16),
        in_specs=[any_] * 4,
        out_specs=vmem,
        scratch_shapes=[
            pltpu.VMEM((total, deep), BF16),
            pltpu.VMEM((2, deep, 2 * width), BF16),
            pltpu.VMEM((2, width, cols), BF16),
            pltpu.VMEM((deep, width), BF16),
            pltpu.VMEM((deep, width), BF16),
            pltpu.VMEM((2, total, 2 * width), F32),
            pltpu.VMEM((2, quarters, 2 * width), BF16),
            pltpu.VMEM((2, quarters, 2 * width), BF16),
            pltpu.VMEM((2, 2, quarters, 2 * width), BF16),
            pltpu.VMEM((2, 2, quarters, 2 * width), BF16),
            pltpu.VMEM((total, 2 * width), BF16),
            pltpu.VMEM((total, cols), F32),
            pltpu.VMEM((2, total // 2, cols), BF16),
            pltpu.VMEM((2, total // 2, cols), BF16),
            pltpu.VMEM((2, max(1, WIDE_HOPS) * block, cols), F32),
            pltpu.VMEM((2, max(1, WIDE_HOPS) * block, cols), F32),
            pltpu.SemaphoreType.DMA((4,)),
            pltpu.SemaphoreType.DMA((n,)),
            pltpu.SemaphoreType.DMA((n,)),
        ],
        compiler_params=pltpu.CompilerParams(
            collective_id=0, has_side_effects=True, vmem_limit_bytes=60 * 1024 * 1024),
    )(tokens, gate_weight, up_weight, down_weight)


def solution(mesh):
    return jax.shard_map(
        body,
        mesh=mesh,
        in_specs=(P(("groups", "grid"), "depth"), P("depth", "grid"), P("depth", "grid"), P("grid", "depth")),
        out_specs=P(("groups", "grid"), "depth"),
        check_vma=False,
    )
```

```python
import functools

import jax
import jax.numpy as jnp
from jax import lax
from jax.experimental import pallas as pl
from jax.experimental.pallas import tpu as pltpu
from jax.sharding import PartitionSpec as P

F32 = jnp.float32
BF16 = jnp.bfloat16

A_ROWS = 4
A_COLS = 2
A_PIECES = A_ROWS * A_COLS
D_PIECES = 4
WIDE_HOPS = 3
GATES = (("M", 1), ("R", 2))
EARLY = 5
DIRECT = 1
SPLIT = False
RANK = {"A": 0, "M": 6, "D": 5, "R": 1, "S": 2, "F": 1, "N": 5, "Z": 4}


class Plan:
    def __init__(self, chips, block):
        self.S = chips // 2
        self.block = block
        self.total = block * chips

    def off(self, s):
        return 0 if s == 0 else self.block * (2 * s - 1)

    def rows(self, s):
        return self.block if s in (0, self.S) else 2 * self.block

    def direct(self, s):
        return s > self.S - DIRECT

    def order(self):
        early = min(EARLY, self.S)
        return list(range(early)) + list(range(self.S, early - 1, -1))

    def pieces(self, s, way, n):
        if s < self.S:
            return list(range(n))
        return list(range(n // 2)) if way == 0 else list(range(n // 2, n))

    def ops(self):
        S, out = self.S, []
        za, zd = 2.8 / A_PIECES, 2.8 / D_PIECES
        out.append((("A", 0, 0), [], [], [(("a", 1, p), "z", za) for p in range(A_PIECES)], 1.0, RANK["A"]))
        for s in range(1, S + 1):
            for p in range(A_PIECES):
                send = [(("a", s + 1, p), "z", za if s + 1 < S else za / 2)] if s < S else []
                out.append((("A", s, p), [("A", 0, 0)], [("a", s, p)], send, 0.04, RANK["A"]))
        seq = self.order()
        for i, s in enumerate(seq):
            u = self.rows(s) / (2 * self.block)
            deps = [("A", s, p) for p in range(A_PIECES)] if s else [("A", 0, 0)]
            if i:
                deps.append(("M", seq[i - 1]))
            stage, lag = GATES[i > EARLY]
            if i >= lag and not (stage == "R" and self.direct(seq[i - lag])):
                deps.append((stage, seq[i - lag]))
            x = 1.23 * u
            if self.direct(s):
                out.append((("M", s), deps, [], [(("r", s), "x", 2 * x), (("d", s), "x", 2 * x)], 1.0, RANK["M"]))
                out.append((("S", s), [("M", s)], [("r", s), ("d", s)], [(("h", s), "x", 2 * x)], 0.2, RANK["S"]))
                out.append((("N", s), [("S", s)], [("h", s)], [], 0.45, RANK["N"]))
                continue
            if SPLIT:
                out.append((("M", s), deps, [], [(("r", s), "x", x)], 1.0, RANK["M"]))
                out.append((("D", s), [("M", s)], [], [(("d", s), "x", x)], 0.03, RANK["D"]))
            else:
                out.append((("M", s), deps, [], [(("r", s), "x", x), (("d", s), "x", x)], 1.0, RANK["M"]))
            out.append((("R", s), [("M", s)], [("r", s)], [(("e", s), "x", x)], 0.05, RANK["R"]))
            out.append((("S", s), [("R", s)] + [("D", s)] * SPLIT, [("d", s), ("e", s)], [(("h", s), "x", x)], 0.2, RANK["S"]))
            out.append((("F", s), [("S", s)], [("h", s)], [(("f", s), "x", x / 2)], 0.02, RANK["F"]))
            out.append((("N", s), [("F", s)], [("f", s)], [], 0.45, RANK["N"]))
        for s in range(S, -1, -1):
            for p in range(D_PIECES):
                wait = [("z", s, p)] if s < S else []
                wide = 2 if s <= WIDE_HOPS else 1
                send = [(("z", s - 1, p), "z", wide * (zd if s < S else zd / 2))] if s else []
                out.append((("Z", s, p), [("N", s)], wait, send, 0.05, RANK["Z"]))
        return out

    def schedule(self, latency=2.6, start=4.0):
        ops = self.ops()
        done, arrives, free = set(), {}, {"x": 0.0, "z": 0.0}
        now, result = 0.0, []
        while ops:
            best = None
            for k, (name, deps, wait, send, cost, rank) in enumerate(ops):
                if any(d not in done for d in deps) or any(m not in arrives for m in wait):
                    continue
                ready = max([now] + [arrives[m] for m in wait])
                if name[0] == "M":
                    ready = max(ready, start)
                key = (ready, rank, k)
                if best is None or key < best[0]:
                    best = (key, k)
            name, deps, wait, send, cost, rank = ops.pop(best[1])
            now = best[0][0] + cost
            for message, link, length in send:
                free[link] = max(free[link], now) + length
                arrives[message] = free[link] + latency
            done.add(name)
            result.append((name, round(now, 2)))
        return result


def kernel(plan, tok, wg, wu, wd, out, X, W, WD, V, PB, SR, RR, SD, RD, H, O, ZS, ZR, YS, YR,
           local_sem, send_sem, recv_sem):
    S, B = plan.S, plan.block
    ring = 2 * 2 * S
    width = wg.shape[0]
    grid, me = lax.axis_index("grid"), lax.axis_index("depth")
    core = lax.rem(grid, 2)
    other = 1 - core
    partner = {"grid": grid + 1 - 2 * core}
    chip = grid - core
    zway = ({"grid": lax.rem(chip + 2, ring) + other}, {"grid": lax.rem(chip + ring - 2, ring) + other})
    xway = ({"depth": lax.rem(me + 1, 4)}, {"depth": lax.rem(me + 3, 4)})
    across = {"depth": lax.rem(me + 2, 4)}

    numbers, started = {}, []

    def message(key, src, dst, to):
        n = numbers.setdefault(key, len(numbers))
        return pltpu.make_async_remote_copy(
            src_ref=src, dst_ref=dst, send_sem=send_sem.at[n], recv_sem=recv_sem.at[n],
            device_id=to, device_id_type=pl.DeviceIdType.MESH)

    def send(key, src, dst, to):
        m = message(key, src, dst, to)
        m.start()
        started.append(m)

    def arrived(key, dst, to):
        message(key, dst, dst, to).wait_recv()

    loads = [
        pltpu.make_async_copy(tok, X.at[pl.ds(0, B)], local_sem.at[0]),
        pltpu.make_async_copy(wg, V.at[pl.ds(0, width)], local_sem.at[1]),
        pltpu.make_async_copy(wu, V.at[pl.ds(width, width)], local_sem.at[2]),
        pltpu.make_async_copy(wd, WD.at[core], local_sem.at[3]),
    ]
    for load in loads:
        load.start()

    barrier = pltpu.get_barrier_semaphore()
    for to in (*zway, *xway, across, partner):
        pl.semaphore_signal(barrier, inc=1, device_id=to, device_id_type=pl.DeviceIdType.MESH)
    pl.semaphore_wait(barrier, 6)

    def a_part(s, way, p):
        size, wide = B // A_ROWS, X.shape[1] // A_COLS
        base = plan.off(s) + (B if way == 1 and 0 < s < S else 0)
        return pl.ds(base + p // A_COLS * size, size), pl.ds(p % A_COLS * wide, wide)

    def a_send(s, p):
        for way in (0, 1):
            if p in plan.pieces(s + 1, way, A_PIECES):
                send(("a", s + 1, way, p), X.at[a_part(s, way, p)], X.at[a_part(s + 1, way, p)], zway[way])

    def op_a(s, p=None):
        if s == 0:
            loads[0].wait()
            for p in range(A_PIECES):
                a_send(0, p)
            for load in loads[1:3]:
                load.wait()

            @pl.loop(0, 2 * width // 128)
            def _(i):
                r = pl.ds(pl.multiple_of(i * 128, 128), 128)
                W[core, :, r] = V[r, :].T

            send(("w",), W.at[core], W.at[core], partner)
            loads[3].wait()
            send(("v",), WD.at[core], WD.at[core], partner)
            return
        for way in (0, 1):
            if p in plan.pieces(s, way, A_PIECES):
                arrived(("a", s, way, p), X.at[a_part(s, way, p)], zway[way])
        if s < S:
            a_send(s, p)

    def quarter(s, k):
        size = plan.rows(s) // 4
        return pl.ds(pl.multiple_of(plan.off(s) + lax.rem(me + k, 4) * size, 16), size)

    def packed(s):
        return pl.ds(plan.off(s) // 4, plan.rows(s) // 4)

    def op_m(s):
        if s == 0:
            arrived(("w",), W.at[other], partner)
        r, q = pl.ds(plan.off(s), plan.rows(s)), packed(s)
        for half in (0, 1):
            PB[half, r, :] = jnp.dot(X[r, :], W[half], preferred_element_type=F32)
            SR[half, q, :] = PB[half, quarter(s, 2), :].astype(BF16)
            send(("r", s, half), SR.at[half, q], RR.at[half, q], across if plan.direct(s) else xway[half])
        for way, half in ((0, 1), (1, 0), (0, 0), (1, 1)):
            if way == half and not plan.direct(s):
                continue
            SD[way, half, q, :] = PB[half, quarter(s, 1 + 2 * way), :].astype(BF16)
            send(("d", s, way, half), SD.at[way, half, q], RD.at[way, half, q], xway[way])

    def op_r(s):
        q = packed(s)
        for way in (0, 1):
            arrived(("r", s, way), RR.at[way, q], xway[way])
            SD[way, way, q, :] = (PB[way, quarter(s, 1 + 2 * way), :] + RR[way, q, :].astype(F32)).astype(BF16)
            send(("d", s, way, way), SD.at[way, way, q], RD.at[way, way, q], xway[way])

    def op_s(s):
        q, mine = packed(s), quarter(s, 0)
        parts = []
        for way in (0, 1):
            for half in (0, 1):
                arrived(("d", s, way, half), RD.at[way, half, q], xway[way])
        for half in (0, 1):
            t = PB[half, mine, :] + RD[0, half, q, :].astype(F32) + RD[1, half, q, :].astype(F32)
            if plan.direct(s):
                arrived(("r", s, half), RR.at[half, q], across)
                t = t + RR[half, q, :].astype(F32)
            gate, up = t[:, :width], t[:, width:]
            parts.append(gate / (1.0 + jnp.exp(-gate)) * up)
        H[mine, :] = jnp.concatenate(parts, axis=1).astype(BF16)
        for way in (0, 1):
            send(("h", s, way), H.at[mine], H.at[mine], xway[way])
        if plan.direct(s):
            send(("f", s), H.at[mine], H.at[mine], across)

    def passed_on(s, way, k):
        size = plan.rows(s) // 4
        if s in (0, S):
            return quarter(s, k) if way == 0 else None
        start = plan.off(s) + lax.rem(me + k, 4) * size + way * (size // 2)
        return pl.ds(pl.multiple_of(start, 16), size // 2)

    def op_f(s):
        for way in (0, 1):
            k = 3 - 2 * way
            arrived(("h", s, way), H.at[quarter(s, k)], xway[way])
            part = passed_on(s, way, k)
            if part is not None:
                send(("f", s, way), H.at[part], H.at[part], xway[way])

    def op_n(s):
        if s == plan.order()[0]:
            arrived(("v",), WD.at[other], partner)
        if plan.direct(s):
            for way in (0, 1):
                arrived(("h", s, way), H.at[quarter(s, 3 - 2 * way)], xway[way])
            arrived(("f", s), H.at[quarter(s, 2)], across)
        else:
            for way in (0, 1):
                part = passed_on(s, way, 2)
                if part is not None:
                    arrived(("f", s, way), H.at[part], xway[way])
        r = pl.ds(plan.off(s), plan.rows(s))
        depth = WD.shape[0] * WD.shape[1]
        O[r, :] = jnp.dot(H[r, :], WD[...].reshape(depth, WD.shape[2]), preferred_element_type=F32)

    def z_place(s, way, p):
        size = B // D_PIECES
        r = pl.ds(s * B + p * size, size)
        return (YS.at[way, r], YR.at[way, r]) if s < WIDE_HOPS else (ZS.at[way, r], ZR.at[way, r])

    def op_z(s, p):
        size = B // D_PIECES
        total = None
        for way in (0, 1):
            if p not in plan.pieces(s, way, D_PIECES):
                continue
            if s == 0:
                base = 0
            else:
                base = plan.off(s) + (B if way == 0 and s < S else 0)
            if total is None or s > 0:
                total = O[pl.ds(base + p * size, size), :]
            if s < S and p in plan.pieces(s + 1, way, D_PIECES):
                got = z_place(s, way, p)[1]
                arrived(("z", s, way, p), got, zway[way])
                total = total + got[...].astype(F32)
            if s > 0:
                src, dst = z_place(s - 1, way, p)
                src[...] = total.astype(src.dtype)
                send(("z", s - 1, way, p), src, dst, zway[way])
        if s == 0:
            out[pl.ds(p * size, size), :] = total.astype(BF16)

    run = {"A": op_a, "M": op_m, "R": op_r, "S": op_s, "F": op_f, "N": op_n, "Z": op_z}
    for (name, *at), _ in plan.schedule():
        run[name](*at)
    for m in started:
        m.wait_send()


def messages(plan):
    S = plan.S
    rings = 2 * ((S - 1) * (A_PIECES + D_PIECES) + (A_PIECES + D_PIECES) // 2)
    return rings + 2 + (S + 1) * 10


def body(tokens, gate_weight, up_weight, down_weight):
    block, deep = tokens.shape
    width, cols = down_weight.shape
    chips = lax.axis_size("grid") // 2
    plan = Plan(chips, block)
    total, quarters = plan.total, plan.total // 4
    vmem, any_ = pl.BlockSpec(memory_space=pltpu.VMEM), pl.BlockSpec(memory_space=pl.ANY)
    n = messages(plan)
    return pl.pallas_call(
        functools.partial(kernel, plan),
        out_shape=jax.ShapeDtypeStruct((block, cols), BF16),
        in_specs=[any_] * 4,
        out_specs=vmem,
        scratch_shapes=[
            pltpu.VMEM((total, deep), BF16),
            pltpu.VMEM((2, deep, 2 * width), BF16),
            pltpu.VMEM((2, width, cols), BF16),
            pltpu.VMEM((2 * width, deep), BF16),
            pltpu.VMEM((2, total, 2 * width), F32),
            pltpu.VMEM((2, quarters, 2 * width), BF16),
            pltpu.VMEM((2, quarters, 2 * width), BF16),
            pltpu.VMEM((2, 2, quarters, 2 * width), BF16),
            pltpu.VMEM((2, 2, quarters, 2 * width), BF16),
            pltpu.VMEM((total, 2 * width), BF16),
            pltpu.VMEM((total, cols), F32),
            pltpu.VMEM((2, total // 2, cols), BF16),
            pltpu.VMEM((2, total // 2, cols), BF16),
            pltpu.VMEM((2, max(1, WIDE_HOPS) * block, cols), F32),
            pltpu.VMEM((2, max(1, WIDE_HOPS) * block, cols), F32),
            pltpu.SemaphoreType.DMA((4,)),
            pltpu.SemaphoreType.DMA((n,)),
            pltpu.SemaphoreType.DMA((n,)),
        ],
        compiler_params=pltpu.CompilerParams(
            collective_id=0, has_side_effects=True, vmem_limit_bytes=60 * 1024 * 1024),
    )(tokens, gate_weight.T, up_weight.T, down_weight)


def solution(mesh):
    return jax.shard_map(
        body,
        mesh=mesh,
        in_specs=(P(("groups", "grid"), "depth"), P("depth", "grid"), P("depth", "grid"), P("grid", "depth")),
        out_specs=P(("groups", "grid"), "depth"),
        check_vma=False,
    )
```

```python
import functools

import jax
import jax.numpy as jnp
from jax import lax
from jax.experimental import pallas as pl
from jax.experimental.pallas import tpu as pltpu
from jax.sharding import PartitionSpec as P

F32 = jnp.float32
BF16 = jnp.bfloat16

A_ROWS = 4
A_COLS = 2
A_PIECES = A_ROWS * A_COLS
D_PIECES = 4
WIDE_HOPS = 3

SEQUENCE = (0, 1, 5, 6, 7, 8, 4, 3, 2)
GATES = (("M", 2), ("R", 2), ("M", 2), ("R", 3), ("R", 3), ("M", 3), ("F", 3), ("F", 3), ("R", 2))
RANK = {"A": 0, "M": 4, "R": 3, "S": 5, "F": 5, "N": 1, "Z": 0}


class Plan:
    def __init__(self, chips, block):
        self.S = chips // 2
        self.block = block
        self.total = block * chips

    def off(self, s):
        return 0 if s == 0 else self.block * (2 * s - 1)

    def rows(self, s):
        return self.block if s in (0, self.S) else 2 * self.block

    def direct(self, s):
        return s == self.S

    def order(self):
        if len(SEQUENCE) == self.S + 1:
            return list(zip(SEQUENCE, GATES))
        return [(s, None) for s in [0, *range(self.S, 0, -1)]]

    def pieces(self, s, way, n):
        if s < self.S:
            return list(range(n))
        return list(range(n // 2)) if way == 0 else list(range(n // 2, n))

    def ops(self):
        S, out = self.S, []
        za, zd = 2.8 / A_PIECES, 2.8 / D_PIECES
        out.append((("A", 0, 0), [], [], [(("a", 1, p), "z", za) for p in range(A_PIECES)], 1.0))
        for s in range(1, S + 1):
            for p in range(A_PIECES):
                send = [(("a", s + 1, p), "z", za if s + 1 < S else za / 2)] if s < S else []
                out.append((("A", s, p), [("A", 0, 0)], [("a", s, p)], send, 0.04))
        order = self.order()
        for i, (s, gate) in enumerate(order):
            x = 1.23 * self.rows(s) / (2 * self.block)
            deps = [("A", s, p) for p in range(A_PIECES)] if s else [("A", 0, 0)]
            if i:
                deps.append(("M", order[i - 1][0], 1))
            if gate and i >= gate[1]:
                stage, t = gate[0], order[i - gate[1]][0]
                if not (stage in "RF" and self.direct(t)):
                    deps += [(stage, t, 0), (stage, t, 1)] if stage in "RFM" else [(stage, t)]
            across = self.direct(s)
            for h in (0, 1):
                send = [(("r", s, h), ("x", h), 2 * x if across else x), (("d", s, 1 - h, h), ("x", 1 - h), x)]
                if across:
                    send.append((("d", s, h, h), ("x", h), x))
                out.append((("M", s, h), [("M", s, 0)] if h else deps, [], send, 0.52))
            parts = [("d", s, w, h) for w in (0, 1) for h in (0, 1)]
            if across:
                send = [(("h", s, w), ("x", w), 2 * x) for w in (0, 1)]
                out.append((("S", s), [("M", s, 1)], parts + [("r", s, 0), ("r", s, 1)], send, 0.2))
                out.append((("N", s), [("S", s)], [("h", s, 0), ("h", s, 1)], [], 0.45))
                continue
            for w in (0, 1):
                out.append((("R", s, w), [("M", s, 1)], [("r", s, w)], [(("d", s, w, w), ("x", w), x)], 0.03))
            send = [(("h", s, w), ("x", w), x) for w in (0, 1)]
            out.append((("S", s), [("R", s, 0), ("R", s, 1)], parts, send, 0.2))
            for w in (0, 1):
                out.append((("F", s, w), [("S", s)], [("h", s, w)], [(("f", s, w), ("x", w), x / 2)], 0.02))
            out.append((("N", s), [("F", s, 0), ("F", s, 1)], [("f", s, 0), ("f", s, 1)], [], 0.45))
        for s in range(S, -1, -1):
            for p in range(D_PIECES):
                wide = 2 if s <= WIDE_HOPS else 1
                send = [(("z", s - 1, p), "z", wide * (zd if s < S else zd / 2))] if s else []
                out.append((("Z", s, p), [("N", s)], [("z", s, p)] if s < S else [], send, 0.05))
        return out

    def schedule(self, latency=2.6, start=4.0):
        ops = self.ops()
        done, arrives, free = set(), {}, {}
        now, result = 0.0, []
        while ops:
            best = None
            for k, (name, deps, wait, send, cost) in enumerate(ops):
                if any(d not in done for d in deps) or any(m not in arrives for m in wait):
                    continue
                ready = max([now] + [arrives[m] for m in wait])
                if name[0] == "M":
                    ready = max(ready, start)
                key = (ready, RANK[name[0]], k)
                if best is None or key < best[0]:
                    best = (key, k)
            name, deps, wait, send, cost = ops.pop(best[1])
            now = best[0][0] + cost
            for message, link, length in send:
                free[link] = max(free.get(link, 0.0), now) + length
                arrives[message] = free[link] + latency
            done.add(name)
            result.append((name, round(now, 2)))
        return result


def kernel(plan, tok, wg, wu, wd, out, X, W, WD, V, PB, SR, RR, SD, RD, H, O, ZS, ZR, YS, YR,
           local_sem, send_sem, recv_sem):
    S, B = plan.S, plan.block
    ring = 2 * 2 * S
    width = wg.shape[0]
    grid, me = lax.axis_index("grid"), lax.axis_index("depth")
    core = lax.rem(grid, 2)
    other = 1 - core
    partner = {"grid": grid + 1 - 2 * core}
    chip = grid - core
    zway = ({"grid": lax.rem(chip + 2, ring) + other}, {"grid": lax.rem(chip + ring - 2, ring) + other})
    xway = ({"depth": lax.rem(me + 1, 4)}, {"depth": lax.rem(me + 3, 4)})
    across = {"depth": lax.rem(me + 2, 4)}

    numbers, started = {}, []

    def message(key, src, dst, to):
        n = numbers.setdefault(key, len(numbers))
        return pltpu.make_async_remote_copy(
            src_ref=src, dst_ref=dst, send_sem=send_sem.at[n], recv_sem=recv_sem.at[n],
            device_id=to, device_id_type=pl.DeviceIdType.MESH)

    def send(key, src, dst, to):
        m = message(key, src, dst, to)
        m.start()
        started.append(m)

    def arrived(key, dst, to):
        message(key, dst, dst, to).wait_recv()

    loads = [
        pltpu.make_async_copy(tok, X.at[pl.ds(0, B)], local_sem.at[0]),
        pltpu.make_async_copy(wg, V.at[pl.ds(0, width)], local_sem.at[1]),
        pltpu.make_async_copy(wu, V.at[pl.ds(width, width)], local_sem.at[2]),
        pltpu.make_async_copy(wd, WD.at[core], local_sem.at[3]),
    ]
    for load in loads:
        load.start()

    barrier = pltpu.get_barrier_semaphore()
    for to in (*zway, *xway, across, partner):
        pl.semaphore_signal(barrier, inc=1, device_id=to, device_id_type=pl.DeviceIdType.MESH)
    pl.semaphore_wait(barrier, 6)

    def a_part(s, way, p):
        size, wide = B // A_ROWS, X.shape[1] // A_COLS
        base = plan.off(s) + (B if way == 1 and 0 < s < S else 0)
        return pl.ds(base + p // A_COLS * size, size), pl.ds(p % A_COLS * wide, wide)

    def a_send(s, p):
        for way in (0, 1):
            if p in plan.pieces(s + 1, way, A_PIECES):
                send(("a", s + 1, way, p), X.at[a_part(s, way, p)], X.at[a_part(s + 1, way, p)], zway[way])

    def op_a(s, p=None):
        if s == 0:
            loads[0].wait()
            for p in range(A_PIECES):
                a_send(0, p)
            for load in loads[1:3]:
                load.wait()

            @pl.loop(0, 2 * width // 128)
            def _(i):
                r = pl.ds(pl.multiple_of(i * 128, 128), 128)
                W[core, :, r] = V[r, :].T

            send(("w",), W.at[core], W.at[core], partner)
            loads[3].wait()
            send(("v",), WD.at[core], WD.at[core], partner)
            return
        for way in (0, 1):
            if p in plan.pieces(s, way, A_PIECES):
                arrived(("a", s, way, p), X.at[a_part(s, way, p)], zway[way])
        if s < S:
            a_send(s, p)

    def quarter(s, k):
        size = plan.rows(s) // 4
        return pl.ds(pl.multiple_of(plan.off(s) + lax.rem(me + k, 4) * size, 16), size)

    def packed(s):
        return pl.ds(plan.off(s) // 4, plan.rows(s) // 4)

    pending = {"w", "v"}

    def op_m(s, half):
        if "w" in pending:
            pending.remove("w")
            arrived(("w",), W.at[other], partner)
        r, q = pl.ds(plan.off(s), plan.rows(s)), packed(s)
        PB[half, r, :] = jnp.dot(X[r, :], W[half], preferred_element_type=F32)
        SR[half, q, :] = PB[half, quarter(s, 2), :].astype(BF16)
        send(("r", s, half), SR.at[half, q], RR.at[half, q], across if plan.direct(s) else xway[half])
        for way in (1 - half, half) if plan.direct(s) else (1 - half,):
            SD[way, half, q, :] = PB[half, quarter(s, 1 + 2 * way), :].astype(BF16)
            send(("d", s, way, half), SD.at[way, half, q], RD.at[way, half, q], xway[way])

    def op_r(s, way):
        q = packed(s)
        arrived(("r", s, way), RR.at[way, q], xway[way])
        SD[way, way, q, :] = (PB[way, quarter(s, 1 + 2 * way), :] + RR[way, q, :].astype(F32)).astype(BF16)
        send(("d", s, way, way), SD.at[way, way, q], RD.at[way, way, q], xway[way])

    def op_s(s):
        q, mine = packed(s), quarter(s, 0)
        parts = []
        for way in (0, 1):
            for half in (0, 1):
                arrived(("d", s, way, half), RD.at[way, half, q], xway[way])
        for half in (0, 1):
            t = PB[half, mine, :] + RD[0, half, q, :].astype(F32) + RD[1, half, q, :].astype(F32)
            if plan.direct(s):
                arrived(("r", s, half), RR.at[half, q], across)
                t = t + RR[half, q, :].astype(F32)
            gate, up = t[:, :width], t[:, width:]
            parts.append(gate / (1.0 + jnp.exp(-gate)) * up)
        H[mine, :] = jnp.concatenate(parts, axis=1).astype(BF16)
        for way in (0, 1):
            send(("h", s, way), H.at[mine], H.at[mine], xway[way])
        if plan.direct(s):
            send(("f", s), H.at[mine], H.at[mine], across)

    def passed_on(s, way, k):
        size = plan.rows(s) // 4
        if s == 0:
            return quarter(s, k) if way == 0 else None
        start = plan.off(s) + lax.rem(me + k, 4) * size + way * (size // 2)
        return pl.ds(pl.multiple_of(start, 16), size // 2)

    def op_f(s, way):
        k = 3 - 2 * way
        arrived(("h", s, way), H.at[quarter(s, k)], xway[way])
        part = passed_on(s, way, k)
        if part is not None:
            send(("f", s, way), H.at[part], H.at[part], xway[way])

    def op_n(s):
        if "v" in pending:
            pending.remove("v")
            arrived(("v",), WD.at[other], partner)
        if plan.direct(s):
            for way in (0, 1):
                arrived(("h", s, way), H.at[quarter(s, 3 - 2 * way)], xway[way])
            arrived(("f", s), H.at[quarter(s, 2)], across)
        else:
            for way in (0, 1):
                part = passed_on(s, way, 2)
                if part is not None:
                    arrived(("f", s, way), H.at[part], xway[way])
        r = pl.ds(plan.off(s), plan.rows(s))
        depth = WD.shape[0] * WD.shape[1]
        O[r, :] = jnp.dot(H[r, :], WD[...].reshape(depth, WD.shape[2]), preferred_element_type=F32)

    def z_place(s, way, p):
        size = B // D_PIECES
        r = pl.ds(s * B + p * size, size)
        return (YS.at[way, r], YR.at[way, r]) if s < WIDE_HOPS else (ZS.at[way, r], ZR.at[way, r])

    def op_z(s, p):
        size = B // D_PIECES
        total = None
        for way in (0, 1):
            if p not in plan.pieces(s, way, D_PIECES):
                continue
            if s == 0:
                base = 0
            else:
                base = plan.off(s) + (B if way == 0 and s < S else 0)
            if total is None or s > 0:
                total = O[pl.ds(base + p * size, size), :]
            if s < S and p in plan.pieces(s + 1, way, D_PIECES):
                got = z_place(s, way, p)[1]
                arrived(("z", s, way, p), got, zway[way])
                total = total + got[...].astype(F32)
            if s > 0:
                src, dst = z_place(s - 1, way, p)
                src[...] = total.astype(src.dtype)
                send(("z", s - 1, way, p), src, dst, zway[way])
        if s == 0:
            out[pl.ds(p * size, size), :] = total.astype(BF16)

    run = {"A": op_a, "M": op_m, "R": op_r, "S": op_s, "F": op_f, "N": op_n, "Z": op_z}
    for (name, *at), _ in plan.schedule():
        run[name](*at)
    for m in started:
        m.wait_send()


def messages(plan):
    S = plan.S
    rings = 2 * ((S - 1) * (A_PIECES + D_PIECES) + (A_PIECES + D_PIECES) // 2)
    return rings + 2 + (S + 1) * 10


def body(tokens, gate_weight, up_weight, down_weight):
    block, deep = tokens.shape
    width, cols = down_weight.shape
    chips = lax.axis_size("grid") // 2
    plan = Plan(chips, block)
    total, quarters = plan.total, plan.total // 4
    vmem, any_ = pl.BlockSpec(memory_space=pltpu.VMEM), pl.BlockSpec(memory_space=pl.ANY)
    n = messages(plan)
    return pl.pallas_call(
        functools.partial(kernel, plan),
        out_shape=pltpu.VMEM((block, cols), BF16),
        in_specs=[any_] * 4,
        out_specs=vmem,
        scratch_shapes=[
            pltpu.VMEM((total, deep), BF16),
            pltpu.VMEM((2, deep, 2 * width), BF16),
            pltpu.VMEM((2, width, cols), BF16),
            pltpu.VMEM((2 * width, deep), BF16),
            pltpu.VMEM((2, total, 2 * width), F32),
            pltpu.VMEM((2, quarters, 2 * width), BF16),
            pltpu.VMEM((2, quarters, 2 * width), BF16),
            pltpu.VMEM((2, 2, quarters, 2 * width), BF16),
            pltpu.VMEM((2, 2, quarters, 2 * width), BF16),
            pltpu.VMEM((total, 2 * width), BF16),
            pltpu.VMEM((total, cols), F32),
            pltpu.VMEM((2, total // 2, cols), BF16),
            pltpu.VMEM((2, total // 2, cols), BF16),
            pltpu.VMEM((2, max(1, WIDE_HOPS) * block, cols), F32),
            pltpu.VMEM((2, max(1, WIDE_HOPS) * block, cols), F32),
            pltpu.SemaphoreType.DMA((4,)),
            pltpu.SemaphoreType.DMA((n,)),
            pltpu.SemaphoreType.DMA((n,)),
        ],
        compiler_params=pltpu.CompilerParams(
            collective_id=0, has_side_effects=True, vmem_limit_bytes=60 * 1024 * 1024),
    )(tokens, gate_weight.T, up_weight.T, down_weight)


def solution(mesh):
    return jax.shard_map(
        body,
        mesh=mesh,
        in_specs=(P(("groups", "grid"), "depth"), P("depth", "grid"), P("depth", "grid"), P("grid", "depth")),
        out_specs=P(("groups", "grid"), "depth"),
        check_vma=False,
    )
```

```python
import functools
import heapq

import jax
import jax.numpy as jnp
from jax import lax
from jax.experimental import pallas as pl
from jax.experimental.pallas import tpu as pltpu
from jax.sharding import PartitionSpec as P

F32 = jnp.float32
BF16 = jnp.bfloat16

A_ROWS = 4
A_COLS = 2
A_PIECES = A_ROWS * A_COLS
D_PIECES = 4
WIDE_HOPS = 3
CUT = 512

SEQUENCE = (
    (0, 0), (1, 1), (3, 1), (4, 1), (5, 0), (5, 1), (6, 0), (7, 1), (7, 0), (6, 1), (8, 0), (4, 0), (3, 0), (2, 0),
    (2, 1), (1, 0),
)
GATES = (
    ("R", 3), None, ("R", 1), ("S", 3), ("F", 1), ("F", 3), None, ("M", 3), ("M", 4), ("R", 3), ("R", 2), ("F", 3),
    ("N", 4), ("R", 2), ("S", 2), ("M", 3),
)
DIRECT = (
    (0, 0), (1, 0), (1, 1), (2, 0), (2, 1), (3, 0), (3, 1), (4, 0), (4, 1), (8, 0),
)
RANK = {"A": 0, "M": 2, "R": 5, "S": 2, "F": 5, "N": 6, "Z": 0}


class Plan:
    def __init__(self, chips, block):
        self.S = chips // 2
        self.block = block
        self.total = block * chips
        self.blocks = [(0, 0), *((s, w) for s in range(1, self.S) for w in (0, 1)), (self.S, 0)]

    def off(self, b):
        return self.block * self.blocks.index(b)

    def order(self):
        if len(SEQUENCE) == len(self.blocks):
            return list(zip(SEQUENCE, GATES))
        return [(b, None) for b in self.blocks[:1] + self.blocks[:0:-1]]

    def pieces(self, s, way, n):
        if s < self.S:
            return range(n)
        return range(n // 2) if way == 0 else range(n // 2, n)

    def ops(self):
        S, out = self.S, []
        za, zd, x = 2.8 / A_PIECES, 2.8 / D_PIECES, 0.615
        first = ("A", 0, 0, 0)
        out.append((first, [], [], [(("a", 1, w, p), ("z", w), za) for p in range(A_PIECES) for w in (0, 1)], 0.9))
        for s in range(1, S + 1):
            for p in range(A_PIECES):
                for w in (0, 1):
                    if p in self.pieces(s, w, A_PIECES):
                        on = s < S and p in self.pieces(s + 1, w, A_PIECES)
                        send = [(("a", s + 1, w, p), ("z", w), za)] if on else []
                        out.append((("A", s, w, p), [first], [("a", s, w, p)], send, 0.03))
        order = self.order()
        for i, (b, gate) in enumerate(order):
            s, w = b
            if s == 0:
                deps = [first]
            else:
                ways = (w,) if s < S else (0, 1)
                deps = [("A", s, v, p) for v in ways for p in self.pieces(s, v, A_PIECES)]
            if i:
                deps.append(("M", order[i - 1][0], 1, 1))
            if gate and i >= gate[1]:
                stage, t = gate[0], order[i - gate[1]][0]
                if stage == "M":
                    deps.append(("M", t, 1, 1))
                elif stage in "SN":
                    deps.append((stage, t))
                elif t not in DIRECT:
                    deps += [("R", t, 0), ("R", t, 1)] if stage == "R" else [("F", t)]
            across = b in DIRECT
            for h in (0, 1):
                send = [(("r", b, h), ("x", h), 2 * x if across else x), (("d", b, 1 - h, h), ("x", 1 - h), x)]
                if across:
                    send.append((("d", b, h, h), ("x", h), x))
                out.append((("M", b, h, 0), [("M", b, 0, 1)] if h else deps, [], [], 0.29))
                out.append((("M", b, h, 1), [("M", b, h, 0)], [], send, 0.24))
            parts = [("d", b, v, h) for v in (0, 1) for h in (0, 1)]
            if across:
                send = [(("h", b, v), ("x", v), 2 * x) for v in (0, 1)]
                out.append((("S", b), [("M", b, 1, 1)], parts + [("r", b, 0), ("r", b, 1)], send, 0.12))
                out.append((("N", b), [("S", b)], [("h", b, 0), ("h", b, 1)], [], 0.45))
                continue
            for v in (0, 1):
                out.append((("R", b, v), [("M", b, 1, 1)], [("r", b, v)], [(("d", b, v, v), ("x", v), x)], 0.03))
            send = [(("h", b, v), ("x", v), x) for v in (0, 1)]
            out.append((("S", b), [("R", b, 0), ("R", b, 1)], parts, send, 0.12))
            out.append((("F", b), [("S", b)], [("h", b, w)], [(("f", b), ("x", w), x)], 0.02))
            out.append((("N", b), [("F", b)], [("f", b), ("h", b, 1 - w)], [], 0.45))
        for s in range(S, 0, -1):
            for p in range(D_PIECES):
                for w in (0, 1):
                    if p in self.pieces(s, w, D_PIECES):
                        wait = [("z", s, w, p)] if s < S and p in self.pieces(s + 1, w, D_PIECES) else []
                        send = [(("z", s - 1, w, p), ("z", w), 2 * zd if s <= WIDE_HOPS else zd)]
                        out.append((("Z", s, w, p), [("N", (s, 1 - w if s < S else 0))], wait, send, 0.04))
        for p in range(D_PIECES):
            out.append((("Z", 0, 0, p), [("N", (0, 0))], [("z", 0, 0, p), ("z", 0, 1, p)], [], 0.05))
        return out

    def schedule(self, latency=2.6, start=4.0):
        ops = self.ops()
        left = [len(op[1]) + len(op[2]) for op in ops]
        ready, free, users = [0.0] * len(ops), {}, {}
        for i, op in enumerate(ops):
            for key in op[1] + op[2]:
                users.setdefault(key, []).append(i)
        later, now_ready, now, names = [], [], 0.0, []

        def enter(i):
            at = max(ready[i], start) if ops[i][0][0] == "M" else ready[i]
            heapq.heappush(later, (at, RANK[ops[i][0][0]], i))

        for i in range(len(ops)):
            if not left[i]:
                enter(i)
        while later or now_ready:
            while later and later[0][0] <= now:
                _, rank, i = heapq.heappop(later)
                heapq.heappush(now_ready, (rank, i))
            if not now_ready:
                now = later[0][0]
                continue
            name, _, _, sends, cost = ops[heapq.heappop(now_ready)[1]]
            now += cost
            names.append((name, now))
            known = [(name, 0.0)]
            for key, link, length in sends:
                free[link] = max(free.get(link, 0.0), now) + length
                known.append((key, free[link] + latency))
            for key, at in known:
                for i in users.get(key, ()):
                    left[i] -= 1
                    ready[i] = max(ready[i], at)
                    if not left[i]:
                        enter(i)
        return names


def kernel(plan, tok, wg, wu, wd, out, X, W, WD, V, PB, SR, RR, SD, RD, H, O, ZS, ZR, YS, YR,
           local_sem, send_sem, recv_sem):
    S, B = plan.S, plan.block
    ring = 2 * 2 * S
    width = wg.shape[0]
    grid, me = lax.axis_index("grid"), lax.axis_index("depth")
    core = lax.rem(grid, 2)
    other = 1 - core
    partner = {"grid": grid + 1 - 2 * core}
    chip = grid - core
    zway = ({"grid": lax.rem(chip + 2, ring) + other}, {"grid": lax.rem(chip + ring - 2, ring) + other})
    xway = ({"depth": lax.rem(me + 1, 4)}, {"depth": lax.rem(me + 3, 4)})
    across = {"depth": lax.rem(me + 2, 4)}

    numbers, started = {}, []

    def message(key, src, dst, to):
        n = numbers.setdefault(key, len(numbers))
        return pltpu.make_async_remote_copy(
            src_ref=src, dst_ref=dst, send_sem=send_sem.at[n], recv_sem=recv_sem.at[n],
            device_id=to, device_id_type=pl.DeviceIdType.MESH)

    def send(key, src, dst, to):
        m = message(key, src, dst, to)
        m.start()
        started.append(m)

    def arrived(key, dst, to):
        message(key, dst, dst, to).wait_recv()

    loads = [
        pltpu.make_async_copy(tok, X.at[pl.ds(0, B)], local_sem.at[0]),
        pltpu.make_async_copy(wg, V.at[pl.ds(0, width)], local_sem.at[1]),
        pltpu.make_async_copy(wu, V.at[pl.ds(width, width)], local_sem.at[2]),
        pltpu.make_async_copy(wd, WD.at[core], local_sem.at[3]),
    ]
    for load in loads:
        load.start()

    barrier = pltpu.get_barrier_semaphore()
    for to in (*zway, *xway, across, partner):
        pl.semaphore_signal(barrier, inc=1, device_id=to, device_id_type=pl.DeviceIdType.MESH)
    pl.semaphore_wait(barrier, 6)

    def a_part(s, way, p):
        size, wide = B // A_ROWS, X.shape[1] // A_COLS
        base = plan.off((s, way if 0 < s < S else 0))
        return pl.ds(base + p // A_COLS * size, size), pl.ds(p % A_COLS * wide, wide)

    def a_send(s, way, p):
        if s < S and p in plan.pieces(s + 1, way, A_PIECES):
            send(("a", s + 1, way, p), X.at[a_part(s, way, p)], X.at[a_part(s + 1, way, p)], zway[way])

    def op_a(s, way, p):
        if s == 0:
            loads[0].wait()
            for p in range(A_PIECES):
                for way in (0, 1):
                    a_send(0, way, p)
            for load in loads[1:3]:
                load.wait()

            @pl.loop(0, 2 * width // 128)
            def _(i):
                r = pl.ds(pl.multiple_of(i * 128, 128), 128)
                W[core, :, r] = V[r, :].T

            send(("w",), W.at[core], W.at[core], partner)
            loads[3].wait()
            send(("v",), WD.at[core], WD.at[core], partner)
            return
        arrived(("a", s, way, p), X.at[a_part(s, way, p)], zway[way])
        a_send(s, way, p)

    size = B // 4

    def quarter(b, k):
        return pl.ds(pl.multiple_of(plan.off(b) + lax.rem(me + k, 4) * size, 16), size)

    def packed(b):
        return pl.ds(plan.off(b) // 4, size)

    pending = {"w", "v"}

    def op_m(b, half, part):
        if "w" in pending:
            pending.remove("w")
            arrived(("w",), W.at[other], partner)
        r, q = pl.ds(plan.off(b), B), packed(b)
        cut = min(CUT, width)
        cols = pl.ds(0, cut) if part == 0 else pl.ds(cut, 2 * width - cut)
        PB[half, r, cols] = jnp.dot(X[r, :], W[half, :, cols], preferred_element_type=F32)
        if part == 0:
            return
        SR[half, q, :] = PB[half, quarter(b, 2), :].astype(BF16)
        send(("r", b, half), SR.at[half, q], RR.at[half, q], across if b in DIRECT else xway[half])
        for way in (1 - half, half) if b in DIRECT else (1 - half,):
            SD[way, half, q, :] = PB[half, quarter(b, 1 + 2 * way), :].astype(BF16)
            send(("d", b, way, half), SD.at[way, half, q], RD.at[way, half, q], xway[way])

    def op_r(b, way):
        q = packed(b)
        arrived(("r", b, way), RR.at[way, q], xway[way])
        SD[way, way, q, :] = (PB[way, quarter(b, 1 + 2 * way), :] + RR[way, q, :].astype(F32)).astype(BF16)
        send(("d", b, way, way), SD.at[way, way, q], RD.at[way, way, q], xway[way])

    def op_s(b):
        q, mine = packed(b), quarter(b, 0)
        parts = []
        for way in (0, 1):
            for half in (0, 1):
                arrived(("d", b, way, half), RD.at[way, half, q], xway[way])
        for half in (0, 1):
            t = PB[half, mine, :] + RD[0, half, q, :].astype(F32) + RD[1, half, q, :].astype(F32)
            if b in DIRECT:
                arrived(("r", b, half), RR.at[half, q], across)
                t = t + RR[half, q, :].astype(F32)
            gate, up = t[:, :width], t[:, width:]
            parts.append(gate / (1.0 + jnp.exp(-gate)) * up)
        H[mine, :] = jnp.concatenate(parts, axis=1).astype(BF16)
        for way in (0, 1):
            send(("h", b, way), H.at[mine], H.at[mine], xway[way])
        if b in DIRECT:
            send(("f", b), H.at[mine], H.at[mine], across)

    def op_f(b):
        way = b[1]
        rows = H.at[quarter(b, 3 - 2 * way)]
        arrived(("h", b, way), rows, xway[way])
        send(("f", b), rows, rows, xway[way])

    def op_n(b):
        if "v" in pending:
            pending.remove("v")
            arrived(("v",), WD.at[other], partner)
        for way in (0, 1):
            if b in DIRECT or way != b[1]:
                arrived(("h", b, way), H.at[quarter(b, 3 - 2 * way)], xway[way])
        arrived(("f", b), H.at[quarter(b, 2)], across if b in DIRECT else xway[b[1]])
        r = pl.ds(plan.off(b), B)
        depth = WD.shape[0] * WD.shape[1]
        O[r, :] = jnp.dot(H[r, :], WD[...].reshape(depth, WD.shape[2]), preferred_element_type=F32)

    def z_place(s, way, p):
        size = B // D_PIECES
        r = pl.ds(s * B + p * size, size)
        return (YS.at[way, r], YR.at[way, r]) if s < WIDE_HOPS else (ZS.at[way, r], ZR.at[way, r])

    def op_z(s, way, p):
        rows = B // D_PIECES
        total = O[pl.ds(plan.off((s, 1 - way if 0 < s < S else 0)) + p * rows, rows), :]
        for v in (0, 1) if s == 0 else (way,):
            if s < S and p in plan.pieces(s + 1, v, D_PIECES):
                got = z_place(s, v, p)[1]
                arrived(("z", s, v, p), got, zway[v])
                total = total + got[...].astype(F32)
        if s == 0:
            out[pl.ds(p * rows, rows), :] = total.astype(BF16)
            return
        src, dst = z_place(s - 1, way, p)
        src[...] = total.astype(src.dtype)
        send(("z", s - 1, way, p), src, dst, zway[way])

    run = {"A": op_a, "M": op_m, "R": op_r, "S": op_s, "F": op_f, "N": op_n, "Z": op_z}
    for (name, *at), _ in plan.schedule():
        run[name](*at)
    for m in started:
        m.wait_send()


def messages(plan):
    S = plan.S
    rings = 2 * ((S - 1) * (A_PIECES + D_PIECES) + (A_PIECES + D_PIECES) // 2)
    return rings + 2 + 2 * S * 9


def body(tokens, gate_weight, up_weight, down_weight):
    block, deep = tokens.shape
    width, cols = down_weight.shape
    chips = lax.axis_size("grid") // 2
    plan = Plan(chips, block)
    total, quarters = plan.total, plan.total // 4
    vmem, any_ = pl.BlockSpec(memory_space=pltpu.VMEM), pl.BlockSpec(memory_space=pl.ANY)
    n = messages(plan)
    return pl.pallas_call(
        functools.partial(kernel, plan),
        out_shape=pltpu.VMEM((block, cols), BF16),
        in_specs=[any_] * 4,
        out_specs=vmem,
        scratch_shapes=[
            pltpu.VMEM((total, deep), BF16),
            pltpu.VMEM((2, deep, 2 * width), BF16),
            pltpu.VMEM((2, width, cols), BF16),
            pltpu.VMEM((2 * width, deep), BF16),
            pltpu.VMEM((2, total, 2 * width), F32),
            pltpu.VMEM((2, quarters, 2 * width), BF16),
            pltpu.VMEM((2, quarters, 2 * width), BF16),
            pltpu.VMEM((2, 2, quarters, 2 * width), BF16),
            pltpu.VMEM((2, 2, quarters, 2 * width), BF16),
            pltpu.VMEM((total, 2 * width), BF16),
            pltpu.VMEM((total, cols), F32),
            pltpu.VMEM((2, total // 2, cols), BF16),
            pltpu.VMEM((2, total // 2, cols), BF16),
            pltpu.VMEM((2, max(1, WIDE_HOPS) * block, cols), F32),
            pltpu.VMEM((2, max(1, WIDE_HOPS) * block, cols), F32),
            pltpu.SemaphoreType.DMA((4,)),
            pltpu.SemaphoreType.DMA((n,)),
            pltpu.SemaphoreType.DMA((n,)),
        ],
        compiler_params=pltpu.CompilerParams(
            collective_id=0, has_side_effects=True, vmem_limit_bytes=60 * 1024 * 1024),
    )(tokens, gate_weight.T, up_weight.T, down_weight)


def solution(mesh):
    return jax.shard_map(
        body,
        mesh=mesh,
        in_specs=(P(("groups", "grid"), "depth"), P("depth", "grid"), P("depth", "grid"), P("grid", "depth")),
        out_specs=P(("groups", "grid"), "depth"),
        check_vma=False,
    )
```

```python
import functools
import heapq

import jax
import jax.numpy as jnp
from jax import lax
from jax.experimental import pallas as pl
from jax.experimental.pallas import tpu as pltpu
from jax.sharding import PartitionSpec as P

F32 = jnp.float32
BF16 = jnp.bfloat16

A_ROWS = 4
A_COLS = 2
A_PIECES = A_ROWS * A_COLS
D_PIECES = 4
WIDE_HOPS = 2

SEQUENCE = (
    (0, 0), (1, 1), (3, 1), (4, 1), (5, 1), (5, 0), (6, 0), (7, 1), (7, 0), (6, 1), (8, 0), (4, 0), (3, 0), (2, 1),
    (2, 0), (1, 0),
)
GATES = (
    ("R", 1), ("F", 2), ("S", 3), ("M", 2), ("N", 3), ("M", 3), None, ("M", 4), None, ("R", 2), ("R", 4), ("F", 3),
    ("N", 4), ("N", 4), ("N", 4), ("S", 1),
)
DIRECT = (
    (0, 0), (1, 0), (1, 1), (2, 0), (2, 1), (3, 0), (3, 1), (4, 0), (4, 1), (8, 0),
)
RANK = {"A": 0, "M": 4, "R": 2, "S": 6, "F": 3, "N": 5, "Z": 3}


class Plan:
    def __init__(self, chips, block):
        self.S = chips // 2
        self.block = block
        self.total = block * chips
        self.blocks = [(0, 0), *((s, w) for s in range(1, self.S) for w in (0, 1)), (self.S, 0)]

    def off(self, b):
        return self.block * self.blocks.index(b)

    def order(self):
        if len(SEQUENCE) == len(self.blocks):
            return list(zip(SEQUENCE, GATES))
        return [(b, None) for b in self.blocks[:1] + self.blocks[:0:-1]]

    def pieces(self, s, way, n):
        if s < self.S:
            return range(n)
        return range(n // 2) if way == 0 else range(n // 2, n)

    def ops(self):
        S, out = self.S, []
        za, zd, x = 2.8 / A_PIECES, 2.8 / D_PIECES, 0.615
        first = ("A", 0, 0, 0)
        out.append((first, [], [], [(("a", 1, w, p), ("z", w), za) for p in range(A_PIECES) for w in (0, 1)], 0.9))
        for s in range(1, S + 1):
            for p in range(A_PIECES):
                for w in (0, 1):
                    if p in self.pieces(s, w, A_PIECES):
                        on = s < S and p in self.pieces(s + 1, w, A_PIECES)
                        send = [(("a", s + 1, w, p), ("z", w), za)] if on else []
                        out.append((("A", s, w, p), [first], [("a", s, w, p)], send, 0.03))
        order = self.order()
        for i, (b, gate) in enumerate(order):
            s, w = b
            if s == 0:
                deps = [first]
            else:
                ways = (w,) if s < S else (0, 1)
                deps = [("A", s, v, p) for v in ways for p in self.pieces(s, v, A_PIECES)]
            if i:
                deps.append(("M", order[i - 1][0], 1))
            if gate and i >= gate[1]:
                stage, t = gate[0], order[i - gate[1]][0]
                if stage == "M":
                    deps.append(("M", t, 1))
                elif stage in "SN":
                    deps.append((stage, t))
                elif t not in DIRECT:
                    deps += [("R", t, 0), ("R", t, 1)] if stage == "R" else [("F", t)]
            across = b in DIRECT
            for h in (0, 1):
                send = [(("r", b, h), ("x", h), 2 * x if across else x), (("d", b, 1 - h, h), ("x", 1 - h), x)]
                if across:
                    send.append((("d", b, h, h), ("x", h), x))
                out.append((("M", b, h), [("M", b, 0)] if h else deps, [], send, 0.5))
            parts = [("d", b, v, h) for v in (0, 1) for h in (0, 1)]
            if across:
                send = [(("h", b, v), ("x", v), 2 * x) for v in (0, 1)]
                out.append((("S", b), [("M", b, 1)], parts + [("r", b, 0), ("r", b, 1)], send, 0.25))
                out.append((("N", b), [("S", b)], [("h", b, 0), ("h", b, 1)], [], 0.45))
                continue
            for v in (0, 1):
                out.append((("R", b, v), [("M", b, 1)], [("r", b, v)], [(("d", b, v, v), ("x", v), x)], 0.03))
            send = [(("h", b, v), ("x", v), x) for v in (0, 1)]
            out.append((("S", b), [("R", b, 0), ("R", b, 1)], parts, send, 0.17))
            out.append((("F", b), [("S", b)], [("h", b, w)], [(("f", b), ("x", w), x)], 0.02))
            out.append((("N", b), [("F", b)], [("f", b), ("h", b, 1 - w)], [], 0.45))
        for s in range(S, 0, -1):
            for p in range(D_PIECES):
                for w in (0, 1):
                    if p in self.pieces(s, w, D_PIECES):
                        wait = [("z", s, w, p)] if s < S and p in self.pieces(s + 1, w, D_PIECES) else []
                        send = [(("z", s - 1, w, p), ("z", w), 2 * zd if s <= WIDE_HOPS else zd)]
                        out.append((("Z", s, w, p), [("N", (s, 1 - w if s < S else 0))], wait, send, 0.04))
        for p in range(D_PIECES):
            out.append((("Z", 0, 0, p), [("N", (0, 0))], [("z", 0, 0, p), ("z", 0, 1, p)], [], 0.05))
        return out

    def schedule(self, latency=2.6, start=4.0):
        ops = self.ops()
        left = [len(op[1]) + len(op[2]) for op in ops]
        ready, free, users = [0.0] * len(ops), {}, {}
        for i, op in enumerate(ops):
            for key in op[1] + op[2]:
                users.setdefault(key, []).append(i)
        later, now_ready, now, names = [], [], 0.0, []

        def enter(i):
            at = max(ready[i], start) if ops[i][0][0] == "M" else ready[i]
            heapq.heappush(later, (at, RANK[ops[i][0][0]], i))

        for i in range(len(ops)):
            if not left[i]:
                enter(i)
        while later or now_ready:
            while later and later[0][0] <= now:
                _, rank, i = heapq.heappop(later)
                heapq.heappush(now_ready, (rank, i))
            if not now_ready:
                now = later[0][0]
                continue
            name, _, _, sends, cost = ops[heapq.heappop(now_ready)[1]]
            now += cost
            names.append((name, now))
            known = [(name, 0.0)]
            for key, link, length in sends:
                free[link] = max(free.get(link, 0.0), now) + length
                known.append((key, free[link] + latency))
            for key, at in known:
                for i in users.get(key, ()):
                    left[i] -= 1
                    ready[i] = max(ready[i], at)
                    if not left[i]:
                        enter(i)
        return names


def kernel(plan, tok, wg, wu, wd, out, X, W, WD, V, PB, SR, RR, SD, RD, H, O, ZS, ZR, YS, YR,
           local_sem, send_sem, recv_sem):
    S, B = plan.S, plan.block
    ring = 2 * 2 * S
    width = wg.shape[0]
    grid, me = lax.axis_index("grid"), lax.axis_index("depth")
    core = lax.rem(grid, 2)
    other = 1 - core
    partner = {"grid": grid + 1 - 2 * core}
    chip = grid - core
    zway = ({"grid": lax.rem(chip + 2, ring) + other}, {"grid": lax.rem(chip + ring - 2, ring) + other})
    xway = ({"depth": lax.rem(me + 1, 4)}, {"depth": lax.rem(me + 3, 4)})
    across = {"depth": lax.rem(me + 2, 4)}

    numbers, started = {}, []

    def message(key, src, dst, to):
        n = numbers.setdefault(key, len(numbers))
        return pltpu.make_async_remote_copy(
            src_ref=src, dst_ref=dst, send_sem=send_sem.at[n], recv_sem=recv_sem.at[n],
            device_id=to, device_id_type=pl.DeviceIdType.MESH)

    def send(key, src, dst, to):
        m = message(key, src, dst, to)
        m.start()
        started.append(m)

    def arrived(key, dst, to):
        message(key, dst, dst, to).wait_recv()

    loads = [
        pltpu.make_async_copy(tok, X.at[pl.ds(0, B)], local_sem.at[0]),
        pltpu.make_async_copy(wg, V.at[pl.ds(0, width)], local_sem.at[1]),
        pltpu.make_async_copy(wu, V.at[pl.ds(width, width)], local_sem.at[2]),
        pltpu.make_async_copy(wd, WD.at[core], local_sem.at[3]),
    ]
    for load in loads:
        load.start()

    barrier = pltpu.get_barrier_semaphore()
    for to in (*zway, *xway, across, partner):
        pl.semaphore_signal(barrier, inc=1, device_id=to, device_id_type=pl.DeviceIdType.MESH)
    pl.semaphore_wait(barrier, 6)

    def a_part(s, way, p):
        size, wide = B // A_ROWS, X.shape[1] // A_COLS
        base = plan.off((s, way if 0 < s < S else 0))
        return pl.ds(base + p // A_COLS * size, size), pl.ds(p % A_COLS * wide, wide)

    def a_send(s, way, p):
        if s < S and p in plan.pieces(s + 1, way, A_PIECES):
            send(("a", s + 1, way, p), X.at[a_part(s, way, p)], X.at[a_part(s + 1, way, p)], zway[way])

    def op_a(s, way, p):
        if s == 0:
            loads[0].wait()
            for p in range(A_PIECES):
                for way in (0, 1):
                    a_send(0, way, p)
            for load in loads[1:3]:
                load.wait()

            @pl.loop(0, 2 * width // 128)
            def _(i):
                r = pl.ds(pl.multiple_of(i * 128, 128), 128)
                W[core, :, r] = V[r, :].T

            send(("w",), W.at[core], W.at[core], partner)
            loads[3].wait()
            send(("v",), WD.at[core], WD.at[core], partner)
            return
        arrived(("a", s, way, p), X.at[a_part(s, way, p)], zway[way])
        a_send(s, way, p)

    size = B // 4

    def quarter(b, k):
        return pl.ds(pl.multiple_of(plan.off(b) + lax.rem(me + k, 4) * size, 16), size)

    def packed(b):
        return pl.ds(plan.off(b) // 4, size)

    pending = {"w", "v"}

    def op_m(b, half):
        if "w" in pending:
            pending.remove("w")
            arrived(("w",), W.at[other], partner)
        r, q = pl.ds(plan.off(b), B), packed(b)
        PB[half, r, :] = jnp.dot(X[r, :], W[half], preferred_element_type=F32)
        SR[half, q, :] = PB[half, quarter(b, 2), :].astype(BF16)
        send(("r", b, half), SR.at[half, q], RR.at[half, q], across if b in DIRECT else xway[half])
        for way in (1 - half, half) if b in DIRECT else (1 - half,):
            SD[way, half, q, :] = PB[half, quarter(b, 1 + 2 * way), :].astype(BF16)
            send(("d", b, way, half), SD.at[way, half, q], RD.at[way, half, q], xway[way])

    def op_r(b, way):
        q = packed(b)
        arrived(("r", b, way), RR.at[way, q], xway[way])
        SD[way, way, q, :] = (PB[way, quarter(b, 1 + 2 * way), :] + RR[way, q, :].astype(F32)).astype(BF16)
        send(("d", b, way, way), SD.at[way, way, q], RD.at[way, way, q], xway[way])

    def op_s(b):
        q, mine = packed(b), quarter(b, 0)
        parts = []
        for way in (0, 1):
            for half in (0, 1):
                arrived(("d", b, way, half), RD.at[way, half, q], xway[way])
        for half in (0, 1):
            t = PB[half, mine, :] + RD[0, half, q, :].astype(F32) + RD[1, half, q, :].astype(F32)
            if b in DIRECT:
                arrived(("r", b, half), RR.at[half, q], across)
                t = t + RR[half, q, :].astype(F32)
            gate, up = t[:, :width], t[:, width:]
            parts.append(gate / (1.0 + jnp.exp(-gate)) * up)
        H[mine, :] = jnp.concatenate(parts, axis=1).astype(BF16)
        for way in (0, 1):
            send(("h", b, way), H.at[mine], H.at[mine], xway[way])
        if b in DIRECT:
            send(("f", b), H.at[mine], H.at[mine], across)

    def op_f(b):
        way = b[1]
        rows = H.at[quarter(b, 3 - 2 * way)]
        arrived(("h", b, way), rows, xway[way])
        send(("f", b), rows, rows, xway[way])

    def op_n(b):
        if "v" in pending:
            pending.remove("v")
            arrived(("v",), WD.at[other], partner)
        for way in (0, 1):
            if b in DIRECT or way != b[1]:
                arrived(("h", b, way), H.at[quarter(b, 3 - 2 * way)], xway[way])
        arrived(("f", b), H.at[quarter(b, 2)], across if b in DIRECT else xway[b[1]])
        r = pl.ds(plan.off(b), B)
        depth = WD.shape[0] * WD.shape[1]
        O[r, :] = jnp.dot(H[r, :], WD[...].reshape(depth, WD.shape[2]), preferred_element_type=F32)

    def z_place(s, way, p):
        size = B // D_PIECES
        r = pl.ds(s * B + p * size, size)
        return (YS.at[way, r], YR.at[way, r]) if s < WIDE_HOPS else (ZS.at[way, r], ZR.at[way, r])

    def op_z(s, way, p):
        rows = B // D_PIECES
        total = O[pl.ds(plan.off((s, 1 - way if 0 < s < S else 0)) + p * rows, rows), :]
        for v in (0, 1) if s == 0 else (way,):
            if s < S and p in plan.pieces(s + 1, v, D_PIECES):
                got = z_place(s, v, p)[1]
                arrived(("z", s, v, p), got, zway[v])
                total = total + got[...].astype(F32)
        if s == 0:
            out[pl.ds(p * rows, rows), :] = total.astype(BF16)
            return
        src, dst = z_place(s - 1, way, p)
        src[...] = total.astype(src.dtype)
        send(("z", s - 1, way, p), src, dst, zway[way])

    run = {"A": op_a, "M": op_m, "R": op_r, "S": op_s, "F": op_f, "N": op_n, "Z": op_z}
    for (name, *at), _ in plan.schedule():
        run[name](*at)
    for m in started:
        m.wait_send()


def messages(plan):
    S = plan.S
    rings = 2 * ((S - 1) * (A_PIECES + D_PIECES) + (A_PIECES + D_PIECES) // 2)
    return rings + 2 + 2 * S * 9


def body(tokens, gate_weight, up_weight, down_weight):
    block, deep = tokens.shape
    width, cols = down_weight.shape
    chips = lax.axis_size("grid") // 2
    plan = Plan(chips, block)
    total, quarters = plan.total, plan.total // 4
    vmem, any_ = pl.BlockSpec(memory_space=pltpu.VMEM), pl.BlockSpec(memory_space=pl.ANY)
    n = messages(plan)
    return pl.pallas_call(
        functools.partial(kernel, plan),
        out_shape=pltpu.VMEM((block, cols), BF16),
        in_specs=[any_] * 4,
        out_specs=vmem,
        scratch_shapes=[
            pltpu.VMEM((total, deep), BF16),
            pltpu.VMEM((2, deep, 2 * width), BF16),
            pltpu.VMEM((2, width, cols), BF16),
            pltpu.VMEM((2 * width, deep), BF16),
            pltpu.VMEM((2, total, 2 * width), F32),
            pltpu.VMEM((2, quarters, 2 * width), BF16),
            pltpu.VMEM((2, quarters, 2 * width), BF16),
            pltpu.VMEM((2, 2, quarters, 2 * width), BF16),
            pltpu.VMEM((2, 2, quarters, 2 * width), BF16),
            pltpu.VMEM((total, 2 * width), BF16),
            pltpu.VMEM((total, cols), F32),
            pltpu.VMEM((2, total // 2, cols), BF16),
            pltpu.VMEM((2, total // 2, cols), BF16),
            pltpu.VMEM((2, max(1, WIDE_HOPS) * block, cols), F32),
            pltpu.VMEM((2, max(1, WIDE_HOPS) * block, cols), F32),
            pltpu.SemaphoreType.DMA((4,)),
            pltpu.SemaphoreType.DMA((n,)),
            pltpu.SemaphoreType.DMA((n,)),
        ],
        compiler_params=pltpu.CompilerParams(
            collective_id=0, has_side_effects=True, vmem_limit_bytes=60 * 1024 * 1024),
    )(tokens, gate_weight.T, up_weight.T, down_weight)


def solution(mesh):
    return jax.shard_map(
        body,
        mesh=mesh,
        in_specs=(P(("groups", "grid"), "depth"), P("depth", "grid"), P("depth", "grid"), P("grid", "depth")),
        out_specs=P(("groups", "grid"), "depth"),
        check_vma=False,
    )
```

```python
import functools
import heapq

import jax
import jax.numpy as jnp
from jax import lax
from jax.experimental import pallas as pl
from jax.experimental.pallas import tpu as pltpu
from jax.sharding import PartitionSpec as P

F32 = jnp.float32
BF16 = jnp.bfloat16

A_ROWS = 4
A_COLS = 2
A_PIECES = A_ROWS * A_COLS
D_ROWS = 4
D_COLS = 2
D_PIECES = D_ROWS * D_COLS
WIDE_HOPS = 2

SEQUENCE = (
    (0, 0), (1, 1), (3, 1), (4, 1), (5, 1), (6, 1), (6, 0), (7, 1), (7, 0), (5, 0), (8, 0), (4, 0), (3, 0), (2, 1),
    (2, 0), (1, 0),
)
GATES = (
    ("S", 2), ("R", 2), None, None, ("R", 2), ("R", 2), ("F", 3), ("M", 1), ("R", 4), None, ("R", 2), ("F", 3),
    None, ("F", 4), ("S", 3), ("S", 1),
)
DIRECT = (
    (0, 0), (1, 0), (1, 1), (2, 0), (2, 1), (3, 0), (3, 1), (4, 0), (4, 1), (8, 0),
)
RANK = {"A": 2, "M": 2, "R": 4, "S": 3, "F": 5, "N": 4, "Z": 1}


class Plan:
    def __init__(self, chips, block):
        self.S = chips // 2
        self.block = block
        self.total = block * chips
        self.blocks = [(0, 0), *((s, w) for s in range(1, self.S) for w in (0, 1)), (self.S, 0)]

    def off(self, b):
        return self.block * self.blocks.index(b)

    def order(self):
        if len(SEQUENCE) == len(self.blocks):
            return list(zip(SEQUENCE, GATES))
        return [(b, None) for b in self.blocks[:1] + self.blocks[:0:-1]]

    def pieces(self, s, way, n):
        if s < self.S:
            return range(n)
        return range(n // 2) if way == 0 else range(n // 2, n)

    def ops(self):
        S, out = self.S, []
        za, zd, x = 2.8 / A_PIECES, 2.8 / D_PIECES, 0.615
        first = ("A", 0, 0, 0)
        out.append((first, [], [], [(("a", 1, w, p), ("z", w), za) for p in range(A_PIECES) for w in (0, 1)], 0.9))
        for s in range(1, S + 1):
            for p in range(A_PIECES):
                for w in (0, 1):
                    if p in self.pieces(s, w, A_PIECES):
                        on = s < S and p in self.pieces(s + 1, w, A_PIECES)
                        send = [(("a", s + 1, w, p), ("z", w), za)] if on else []
                        out.append((("A", s, w, p), [first], [("a", s, w, p)], send, 0.03))
        order = self.order()
        for i, (b, gate) in enumerate(order):
            s, w = b
            if s == 0:
                deps = [first]
            else:
                ways = (w,) if s < S else (0, 1)
                deps = [("A", s, v, p) for v in ways for p in self.pieces(s, v, A_PIECES)]
            if i:
                deps.append(("M", order[i - 1][0], 1))
            if gate and i >= gate[1]:
                stage, t = gate[0], order[i - gate[1]][0]
                if stage == "M":
                    deps.append(("M", t, 1))
                elif stage in "SN":
                    deps.append((stage, t))
                elif t not in DIRECT:
                    deps += [("R", t, 0), ("R", t, 1)] if stage == "R" else [("F", t)]
            across = b in DIRECT
            for h in (0, 1):
                send = [(("r", b, h), ("x", h), 2 * x if across else x), (("d", b, 1 - h, h), ("x", 1 - h), x)]
                if across:
                    send.append((("d", b, h, h), ("x", h), x))
                out.append((("M", b, h), [("M", b, 0)] if h else deps, [], send, 0.5))
            parts = [("d", b, v, h) for v in (0, 1) for h in (0, 1)]
            if across:
                send = [(("h", b, v), ("x", v), 2 * x) for v in (0, 1)]
                out.append((("S", b), [("M", b, 1)], parts + [("r", b, 0), ("r", b, 1)], send, 0.25))
                out.append((("N", b), [("S", b)], [("h", b, 0), ("h", b, 1)], [], 0.45))
                continue
            for v in (0, 1):
                out.append((("R", b, v), [("M", b, 1)], [("r", b, v)], [(("d", b, v, v), ("x", v), x)], 0.03))
            send = [(("h", b, v), ("x", v), x) for v in (0, 1)]
            out.append((("S", b), [("R", b, 0), ("R", b, 1)], parts, send, 0.17))
            out.append((("F", b), [("S", b)], [("h", b, w)], [(("f", b), ("x", w), x)], 0.02))
            out.append((("N", b), [("F", b)], [("f", b), ("h", b, 1 - w)], [], 0.45))
        for s in range(S, 0, -1):
            for p in range(D_PIECES):
                for w in (0, 1):
                    if p in self.pieces(s, w, D_PIECES):
                        wait = [("z", s, w, p)] if s < S and p in self.pieces(s + 1, w, D_PIECES) else []
                        send = [(("z", s - 1, w, p), ("z", w), 2 * zd if s <= WIDE_HOPS else zd)]
                        out.append((("Z", s, w, p), [("N", (s, 1 - w if s < S else 0))], wait, send, 0.04))
        for p in range(D_PIECES):
            out.append((("Z", 0, 0, p), [("N", (0, 0))], [("z", 0, 0, p), ("z", 0, 1, p)], [], 0.05))
        return out

    def schedule(self, latency=2.6, start=4.0):
        ops = self.ops()
        left = [len(op[1]) + len(op[2]) for op in ops]
        ready, free, users = [0.0] * len(ops), {}, {}
        for i, op in enumerate(ops):
            for key in op[1] + op[2]:
                users.setdefault(key, []).append(i)
        later, now_ready, now, names = [], [], 0.0, []

        def enter(i):
            at = max(ready[i], start) if ops[i][0][0] == "M" else ready[i]
            heapq.heappush(later, (at, RANK[ops[i][0][0]], i))

        for i in range(len(ops)):
            if not left[i]:
                enter(i)
        while later or now_ready:
            while later and later[0][0] <= now:
                _, rank, i = heapq.heappop(later)
                heapq.heappush(now_ready, (rank, i))
            if not now_ready:
                now = later[0][0]
                continue
            name, _, _, sends, cost = ops[heapq.heappop(now_ready)[1]]
            now += cost
            names.append((name, now))
            known = [(name, 0.0)]
            for key, link, length in sends:
                free[link] = max(free.get(link, 0.0), now) + length
                known.append((key, free[link] + latency))
            for key, at in known:
                for i in users.get(key, ()):
                    left[i] -= 1
                    ready[i] = max(ready[i], at)
                    if not left[i]:
                        enter(i)
        return names


def kernel(plan, tok, wg, wu, wd, out, X, W, WD, V, PB, SR, RR, SD, RD, H, O, ZS, ZR, YS, YR,
           local_sem, send_sem, recv_sem):
    S, B = plan.S, plan.block
    ring = 2 * 2 * S
    width = wg.shape[0]
    grid, me = lax.axis_index("grid"), lax.axis_index("depth")
    core = lax.rem(grid, 2)
    other = 1 - core
    partner = {"grid": grid + 1 - 2 * core}
    chip = grid - core
    zway = ({"grid": lax.rem(chip + 2, ring) + other}, {"grid": lax.rem(chip + ring - 2, ring) + other})
    xway = ({"depth": lax.rem(me + 1, 4)}, {"depth": lax.rem(me + 3, 4)})
    across = {"depth": lax.rem(me + 2, 4)}

    numbers, started = {}, []

    def message(key, src, dst, to):
        n = numbers.setdefault(key, len(numbers))
        return pltpu.make_async_remote_copy(
            src_ref=src, dst_ref=dst, send_sem=send_sem.at[n], recv_sem=recv_sem.at[n],
            device_id=to, device_id_type=pl.DeviceIdType.MESH)

    def send(key, src, dst, to):
        m = message(key, src, dst, to)
        m.start()
        started.append(m)

    def arrived(key, dst, to):
        message(key, dst, dst, to).wait_recv()

    loads = [
        pltpu.make_async_copy(tok, X.at[pl.ds(0, B)], local_sem.at[0]),
        pltpu.make_async_copy(wg, V.at[pl.ds(0, width)], local_sem.at[1]),
        pltpu.make_async_copy(wu, V.at[pl.ds(width, width)], local_sem.at[2]),
        pltpu.make_async_copy(wd, WD.at[core], local_sem.at[3]),
    ]
    for load in loads:
        load.start()

    barrier = pltpu.get_barrier_semaphore()
    for to in (*zway, *xway, across, partner):
        pl.semaphore_signal(barrier, inc=1, device_id=to, device_id_type=pl.DeviceIdType.MESH)
    pl.semaphore_wait(barrier, 6)

    def a_part(s, way, p):
        size, wide = B // A_ROWS, X.shape[1] // A_COLS
        base = plan.off((s, way if 0 < s < S else 0))
        return pl.ds(base + p // A_COLS * size, size), pl.ds(p % A_COLS * wide, wide)

    def a_send(s, way, p):
        if s < S and p in plan.pieces(s + 1, way, A_PIECES):
            send(("a", s + 1, way, p), X.at[a_part(s, way, p)], X.at[a_part(s + 1, way, p)], zway[way])

    def op_a(s, way, p):
        if s == 0:
            loads[0].wait()
            for p in range(A_PIECES):
                for way in (0, 1):
                    a_send(0, way, p)
            for load in loads[1:3]:
                load.wait()

            @pl.loop(0, 2 * width // 128)
            def _(i):
                r = pl.ds(pl.multiple_of(i * 128, 128), 128)
                W[core, :, r] = V[r, :].T

            send(("w",), W.at[core], W.at[core], partner)
            loads[3].wait()
            send(("v",), WD.at[core], WD.at[core], partner)
            return
        arrived(("a", s, way, p), X.at[a_part(s, way, p)], zway[way])
        a_send(s, way, p)

    size = B // 4

    def quarter(b, k):
        return pl.ds(pl.multiple_of(plan.off(b) + lax.rem(me + k, 4) * size, 16), size)

    def packed(b):
        return pl.ds(plan.off(b) // 4, size)

    pending = {"w", "v"}

    def op_m(b, half):
        if "w" in pending:
            pending.remove("w")
            arrived(("w",), W.at[other], partner)
        r, q = pl.ds(plan.off(b), B), packed(b)
        PB[half, r, :] = jnp.dot(X[r, :], W[half], preferred_element_type=F32)
        SR[half, q, :] = PB[half, quarter(b, 2), :].astype(BF16)
        send(("r", b, half), SR.at[half, q], RR.at[half, q], across if b in DIRECT else xway[half])
        for way in (1 - half, half) if b in DIRECT else (1 - half,):
            SD[way, half, q, :] = PB[half, quarter(b, 1 + 2 * way), :].astype(BF16)
            send(("d", b, way, half), SD.at[way, half, q], RD.at[way, half, q], xway[way])

    def op_r(b, way):
        q = packed(b)
        arrived(("r", b, way), RR.at[way, q], xway[way])
        SD[way, way, q, :] = (PB[way, quarter(b, 1 + 2 * way), :] + RR[way, q, :].astype(F32)).astype(BF16)
        send(("d", b, way, way), SD.at[way, way, q], RD.at[way, way, q], xway[way])

    def op_s(b):
        q, mine = packed(b), quarter(b, 0)
        parts = []
        for way in (0, 1):
            for half in (0, 1):
                arrived(("d", b, way, half), RD.at[way, half, q], xway[way])
        for half in (0, 1):
            t = PB[half, mine, :] + RD[0, half, q, :].astype(F32) + RD[1, half, q, :].astype(F32)
            if b in DIRECT:
                arrived(("r", b, half), RR.at[half, q], across)
                t = t + RR[half, q, :].astype(F32)
            gate, up = t[:, :width], t[:, width:]
            parts.append(gate / (1.0 + jnp.exp(-gate)) * up)
        H[mine, :] = jnp.concatenate(parts, axis=1).astype(BF16)
        for way in (0, 1):
            send(("h", b, way), H.at[mine], H.at[mine], xway[way])
        if b in DIRECT:
            send(("f", b), H.at[mine], H.at[mine], across)

    def op_f(b):
        way = b[1]
        rows = H.at[quarter(b, 3 - 2 * way)]
        arrived(("h", b, way), rows, xway[way])
        send(("f", b), rows, rows, xway[way])

    def op_n(b):
        if "v" in pending:
            pending.remove("v")
            arrived(("v",), WD.at[other], partner)
        for way in (0, 1):
            if b in DIRECT or way != b[1]:
                arrived(("h", b, way), H.at[quarter(b, 3 - 2 * way)], xway[way])
        arrived(("f", b), H.at[quarter(b, 2)], across if b in DIRECT else xway[b[1]])
        r = pl.ds(plan.off(b), B)
        depth = WD.shape[0] * WD.shape[1]
        O[r, :] = jnp.dot(H[r, :], WD[...].reshape(depth, WD.shape[2]), preferred_element_type=F32)

    def z_part(base, p):
        rows, wide = B // D_ROWS, O.shape[1] // D_COLS
        return pl.ds(base + p // D_COLS * rows, rows), pl.ds(p % D_COLS * wide, wide)

    def z_place(s, way, p):
        r, c = z_part(s * B, p)
        return (YS.at[way, r, c], YR.at[way, r, c]) if s < WIDE_HOPS else (ZS.at[way, r, c], ZR.at[way, r, c])

    def op_z(s, way, p):
        r, c = z_part(plan.off((s, 1 - way if 0 < s < S else 0)), p)
        total = O[r, c]
        for v in (0, 1) if s == 0 else (way,):
            if s < S and p in plan.pieces(s + 1, v, D_PIECES):
                got = z_place(s, v, p)[1]
                arrived(("z", s, v, p), got, zway[v])
                total = total + got[...].astype(F32)
        if s == 0:
            r, c = z_part(0, p)
            out[r, c] = total.astype(BF16)
            return
        src, dst = z_place(s - 1, way, p)
        src[...] = total.astype(src.dtype)
        send(("z", s - 1, way, p), src, dst, zway[way])

    run = {"A": op_a, "M": op_m, "R": op_r, "S": op_s, "F": op_f, "N": op_n, "Z": op_z}
    for (name, *at), _ in plan.schedule():
        if name == "Z" and at[0] == 0:
            for m in started[: -2 * D_PIECES]:
                m.wait_send()
            del started[: -2 * D_PIECES]
        run[name](*at)
    for m in started:
        m.wait_send()


def messages(plan):
    S = plan.S
    rings = 2 * ((S - 1) * (A_PIECES + D_PIECES) + (A_PIECES + D_PIECES) // 2)
    return rings + 2 + 2 * S * 9


def body(tokens, gate_weight, up_weight, down_weight):
    block, deep = tokens.shape
    width, cols = down_weight.shape
    chips = lax.axis_size("grid") // 2
    plan = Plan(chips, block)
    total, quarters = plan.total, plan.total // 4
    vmem, any_ = pl.BlockSpec(memory_space=pltpu.VMEM), pl.BlockSpec(memory_space=pl.ANY)
    n = messages(plan)
    return pl.pallas_call(
        functools.partial(kernel, plan),
        out_shape=pltpu.VMEM((block, cols), BF16),
        in_specs=[any_] * 4,
        out_specs=vmem,
        scratch_shapes=[
            pltpu.VMEM((total, deep), BF16),
            pltpu.VMEM((2, deep, 2 * width), BF16),
            pltpu.VMEM((2, width, cols), BF16),
            pltpu.VMEM((2 * width, deep), BF16),
            pltpu.VMEM((2, total, 2 * width), F32),
            pltpu.VMEM((2, quarters, 2 * width), BF16),
            pltpu.VMEM((2, quarters, 2 * width), BF16),
            pltpu.VMEM((2, 2, quarters, 2 * width), BF16),
            pltpu.VMEM((2, 2, quarters, 2 * width), BF16),
            pltpu.VMEM((total, 2 * width), BF16),
            pltpu.VMEM((total, cols), F32),
            pltpu.VMEM((2, total // 2, cols), BF16),
            pltpu.VMEM((2, total // 2, cols), BF16),
            pltpu.VMEM((2, max(1, WIDE_HOPS) * block, cols), F32),
            pltpu.VMEM((2, max(1, WIDE_HOPS) * block, cols), F32),
            pltpu.SemaphoreType.DMA((4,)),
            pltpu.SemaphoreType.DMA((n,)),
            pltpu.SemaphoreType.DMA((n,)),
        ],
        compiler_params=pltpu.CompilerParams(
            collective_id=0, has_side_effects=True, vmem_limit_bytes=60 * 1024 * 1024),
    )(tokens, gate_weight.T, up_weight.T, down_weight)


def solution(mesh):
    return jax.shard_map(
        body,
        mesh=mesh,
        in_specs=(P(("groups", "grid"), "depth"), P("depth", "grid"), P("depth", "grid"), P("grid", "depth")),
        out_specs=P(("groups", "grid"), "depth"),
        check_vma=False,
    )
```

```python
import functools
import heapq

import jax
import jax.numpy as jnp
from jax import lax
from jax.experimental import pallas as pl
from jax.experimental.pallas import tpu as pltpu
from jax.sharding import PartitionSpec as P

F32 = jnp.float32
BF16 = jnp.bfloat16

LATENCY = {"x": 3.0, "z": 2.6}
A_ROWS = 4
A_COLS = 2
A_PIECES = A_ROWS * A_COLS
D_ROWS = 4
D_COLS = 1
D_PIECES = D_ROWS * D_COLS
WIDE_HOPS = 2

SEQUENCE = (
    (0, 0), (1, 1), (3, 1), (4, 1), (5, 0), (6, 0), (6, 1), (7, 0), (7, 1), (5, 1), (8, 0), (4, 0), (3, 0), (1, 0),
    (2, 0), (2, 1),
)
GATES = (
    ("R", 2), ("R", 1), ("S", 4), ("R", 3), ("F", 4), ("M", 3), ("R", 3), ("R", 4), ("M", 2), ("M", 2), ("R", 2),
    ("F", 3), None, ("R", 4), ("F", 4), ("R", 3),
)
DIRECT = (
    (0, 0), (1, 1), (2, 0), (2, 1), (3, 0), (3, 1), (4, 0), (4, 1), (8, 0),
)
RANK = {"A": 3, "M": 6, "R": 4, "S": 4, "F": 6, "N": 5, "Z": 1}


class Plan:
    def __init__(self, chips, block):
        self.S = chips // 2
        self.block = block
        self.total = block * chips
        self.blocks = [(0, 0), *((s, w) for s in range(1, self.S) for w in (0, 1)), (self.S, 0)]

    def off(self, b):
        return self.block * self.blocks.index(b)

    def order(self):
        if len(SEQUENCE) == len(self.blocks):
            return list(zip(SEQUENCE, GATES))
        return [(b, None) for b in self.blocks[:1] + self.blocks[:0:-1]]

    def pieces(self, s, way, n):
        if s < self.S:
            return range(n)
        return range(n // 2) if way == 0 else range(n // 2, n)

    def ops(self):
        S, out = self.S, []
        za, zd, x = 2.8 / A_PIECES, 2.8 / D_PIECES, 0.615
        first = ("A", 0, 0, 0)
        out.append((first, [], [], [(("a", 1, w, p), ("z", w), za) for p in range(A_PIECES) for w in (0, 1)], 0.9))
        for s in range(1, S + 1):
            for p in range(A_PIECES):
                for w in (0, 1):
                    if p in self.pieces(s, w, A_PIECES):
                        on = s < S and p in self.pieces(s + 1, w, A_PIECES)
                        send = [(("a", s + 1, w, p), ("z", w), za)] if on else []
                        out.append((("A", s, w, p), [first], [("a", s, w, p)], send, 0.03))
        order = self.order()
        for i, (b, gate) in enumerate(order):
            s, w = b
            if s == 0:
                deps = [first]
            else:
                ways = (w,) if s < S else (0, 1)
                deps = [("A", s, v, p) for v in ways for p in self.pieces(s, v, A_PIECES)]
            if i:
                deps.append(("M", order[i - 1][0], 1))
            if gate and i >= gate[1]:
                stage, t = gate[0], order[i - gate[1]][0]
                if stage == "M":
                    deps.append(("M", t, 1))
                elif stage in "SN":
                    deps.append((stage, t))
                elif t not in DIRECT:
                    deps += [("R", t, 0), ("R", t, 1)] if stage == "R" else [("F", t)]
            across = b in DIRECT
            for h in (0, 1):
                send = [(("r", b, h), ("x", h), 2 * x if across else x), (("d", b, 1 - h, h), ("x", 1 - h), x)]
                if across:
                    send.append((("d", b, h, h), ("x", h), x))
                out.append((("M", b, h), [("M", b, 0)] if h else deps, [], send, 0.5))
            parts = [("d", b, v, h) for v in (0, 1) for h in (0, 1)]
            if across:
                send = [(("h", b, v), ("x", v), 2 * x) for v in (0, 1)]
                out.append((("S", b), [("M", b, 1)], parts + [("r", b, 0), ("r", b, 1)], send, 0.25))
                out.append((("N", b), [("S", b)], [("h", b, 0), ("h", b, 1)], [], 0.45))
                continue
            for v in (0, 1):
                out.append((("R", b, v), [("M", b, 1)], [("r", b, v)], [(("d", b, v, v), ("x", v), x)], 0.03))
            send = [(("h", b, v), ("x", v), x) for v in (0, 1)]
            out.append((("S", b), [("R", b, 0), ("R", b, 1)], parts, send, 0.17))
            out.append((("F", b), [("S", b)], [("h", b, w)], [(("f", b), ("x", w), x)], 0.02))
            out.append((("N", b), [("F", b)], [("f", b), ("h", b, 1 - w)], [], 0.45))
        for s in range(S, 0, -1):
            for p in range(D_PIECES):
                for w in (0, 1):
                    if p in self.pieces(s, w, D_PIECES):
                        wait = [("z", s, w, p)] if s < S and p in self.pieces(s + 1, w, D_PIECES) else []
                        send = [(("z", s - 1, w, p), ("z", w), 2 * zd if s <= WIDE_HOPS else zd)]
                        out.append((("Z", s, w, p), [("N", (s, 1 - w if s < S else 0))], wait, send, 0.04))
        for p in range(D_PIECES):
            out.append((("Z", 0, 0, p), [("N", (0, 0))], [("z", 0, 0, p), ("z", 0, 1, p)], [], 0.05))
        return out

    def schedule(self, start=4.0):
        ops = self.ops()
        left = [len(op[1]) + len(op[2]) for op in ops]
        ready, free, users = [0.0] * len(ops), {}, {}
        for i, op in enumerate(ops):
            for key in op[1] + op[2]:
                users.setdefault(key, []).append(i)
        later, now_ready, now, names = [], [], 0.0, []

        def enter(i):
            at = max(ready[i], start) if ops[i][0][0] == "M" else ready[i]
            heapq.heappush(later, (at, RANK[ops[i][0][0]], i))

        for i in range(len(ops)):
            if not left[i]:
                enter(i)
        while later or now_ready:
            while later and later[0][0] <= now:
                _, rank, i = heapq.heappop(later)
                heapq.heappush(now_ready, (rank, i))
            if not now_ready:
                now = later[0][0]
                continue
            name, _, _, sends, cost = ops[heapq.heappop(now_ready)[1]]
            now += cost
            names.append((name, now))
            known = [(name, 0.0)]
            for key, link, length in sends:
                free[link] = max(free.get(link, 0.0), now) + length
                known.append((key, free[link] + LATENCY[link[0]]))
            for key, at in known:
                for i in users.get(key, ()):
                    left[i] -= 1
                    ready[i] = max(ready[i], at)
                    if not left[i]:
                        enter(i)
        return names


def kernel(plan, tok, wg, wu, wd, out, X, W, WD, V, PB, SR, RR, SD, RD, H, O, ZS, ZR, YS, YR,
           local_sem, send_sem, recv_sem):
    S, B = plan.S, plan.block
    ring = 2 * 2 * S
    width = wg.shape[0]
    grid, me = lax.axis_index("grid"), lax.axis_index("depth")
    core = lax.rem(grid, 2)
    other = 1 - core
    partner = {"grid": grid + 1 - 2 * core}
    chip = grid - core
    zway = ({"grid": lax.rem(chip + 2, ring) + other}, {"grid": lax.rem(chip + ring - 2, ring) + other})
    xway = ({"depth": lax.rem(me + 1, 4)}, {"depth": lax.rem(me + 3, 4)})
    across = {"depth": lax.rem(me + 2, 4)}

    numbers, started = {}, []

    def message(key, src, dst, to):
        n = numbers.setdefault(key, len(numbers))
        return pltpu.make_async_remote_copy(
            src_ref=src, dst_ref=dst, send_sem=send_sem.at[n], recv_sem=recv_sem.at[n],
            device_id=to, device_id_type=pl.DeviceIdType.MESH)

    def send(key, src, dst, to):
        m = message(key, src, dst, to)
        m.start()
        started.append(m)

    def arrived(key, dst, to):
        message(key, dst, dst, to).wait_recv()

    loads = [
        pltpu.make_async_copy(tok, X.at[pl.ds(0, B)], local_sem.at[0]),
        pltpu.make_async_copy(wg, V.at[pl.ds(0, width)], local_sem.at[1]),
        pltpu.make_async_copy(wu, V.at[pl.ds(width, width)], local_sem.at[2]),
        pltpu.make_async_copy(wd, WD.at[core], local_sem.at[3]),
    ]
    for load in loads:
        load.start()

    barrier = pltpu.get_barrier_semaphore()
    for to in (*zway, *xway, across, partner):
        pl.semaphore_signal(barrier, inc=1, device_id=to, device_id_type=pl.DeviceIdType.MESH)
    pl.semaphore_wait(barrier, 6)

    def a_part(s, way, p):
        size, wide = B // A_ROWS, X.shape[1] // A_COLS
        base = plan.off((s, way if 0 < s < S else 0))
        return pl.ds(base + p // A_COLS * size, size), pl.ds(p % A_COLS * wide, wide)

    def a_send(s, way, p):
        if s < S and p in plan.pieces(s + 1, way, A_PIECES):
            send(("a", s + 1, way, p), X.at[a_part(s, way, p)], X.at[a_part(s + 1, way, p)], zway[way])

    def op_a(s, way, p):
        if s == 0:
            loads[0].wait()
            for p in range(A_PIECES):
                for way in (0, 1):
                    a_send(0, way, p)
            for load in loads[1:3]:
                load.wait()

            @pl.loop(0, 2 * width // 128)
            def _(i):
                r = pl.ds(pl.multiple_of(i * 128, 128), 128)
                W[core, :, r] = V[r, :].T

            send(("w",), W.at[core], W.at[core], partner)
            loads[3].wait()
            send(("v",), WD.at[core], WD.at[core], partner)
            return
        arrived(("a", s, way, p), X.at[a_part(s, way, p)], zway[way])
        a_send(s, way, p)

    size = B // 4

    def quarter(b, k):
        return pl.ds(pl.multiple_of(plan.off(b) + lax.rem(me + k, 4) * size, 16), size)

    def packed(b):
        return pl.ds(plan.off(b) // 4, size)

    pending = {"w", "v"}

    def op_m(b, half):
        if "w" in pending:
            pending.remove("w")
            arrived(("w",), W.at[other], partner)
        r, q = pl.ds(plan.off(b), B), packed(b)
        PB[half, r, :] = jnp.dot(X[r, :], W[half], preferred_element_type=F32)
        SR[half, q, :] = PB[half, quarter(b, 2), :].astype(BF16)
        send(("r", b, half), SR.at[half, q], RR.at[half, q], across if b in DIRECT else xway[half])
        for way in (1 - half, half) if b in DIRECT else (1 - half,):
            SD[way, half, q, :] = PB[half, quarter(b, 1 + 2 * way), :].astype(BF16)
            send(("d", b, way, half), SD.at[way, half, q], RD.at[way, half, q], xway[way])

    def op_r(b, way):
        q = packed(b)
        arrived(("r", b, way), RR.at[way, q], xway[way])
        SD[way, way, q, :] = (PB[way, quarter(b, 1 + 2 * way), :] + RR[way, q, :].astype(F32)).astype(BF16)
        send(("d", b, way, way), SD.at[way, way, q], RD.at[way, way, q], xway[way])

    def op_s(b):
        q, mine = packed(b), quarter(b, 0)
        parts = []
        for way in (0, 1):
            for half in (0, 1):
                arrived(("d", b, way, half), RD.at[way, half, q], xway[way])
        for half in (0, 1):
            t = PB[half, mine, :] + RD[0, half, q, :].astype(F32) + RD[1, half, q, :].astype(F32)
            if b in DIRECT:
                arrived(("r", b, half), RR.at[half, q], across)
                t = t + RR[half, q, :].astype(F32)
            gate, up = t[:, :width], t[:, width:]
            parts.append(gate / (1.0 + jnp.exp(-gate)) * up)
        H[mine, :] = jnp.concatenate(parts, axis=1).astype(BF16)
        for way in (0, 1):
            send(("h", b, way), H.at[mine], H.at[mine], xway[way])
        if b in DIRECT:
            send(("f", b), H.at[mine], H.at[mine], across)

    def op_f(b):
        way = b[1]
        rows = H.at[quarter(b, 3 - 2 * way)]
        arrived(("h", b, way), rows, xway[way])
        send(("f", b), rows, rows, xway[way])

    def op_n(b):
        if "v" in pending:
            pending.remove("v")
            arrived(("v",), WD.at[other], partner)
        for way in (0, 1):
            if b in DIRECT or way != b[1]:
                arrived(("h", b, way), H.at[quarter(b, 3 - 2 * way)], xway[way])
        arrived(("f", b), H.at[quarter(b, 2)], across if b in DIRECT else xway[b[1]])
        r = pl.ds(plan.off(b), B)
        depth = WD.shape[0] * WD.shape[1]
        O[r, :] = jnp.dot(H[r, :], WD[...].reshape(depth, WD.shape[2]), preferred_element_type=F32)

    def z_part(base, p):
        rows, wide = B // D_ROWS, O.shape[1] // D_COLS
        return pl.ds(base + p // D_COLS * rows, rows), pl.ds(p % D_COLS * wide, wide)

    def z_place(s, way, p):
        r, c = z_part(s * B, p)
        return (YS.at[way, r, c], YR.at[way, r, c]) if s < WIDE_HOPS else (ZS.at[way, r, c], ZR.at[way, r, c])

    def op_z(s, way, p):
        r, c = z_part(plan.off((s, 1 - way if 0 < s < S else 0)), p)
        total = O[r, c]
        for v in (0, 1) if s == 0 else (way,):
            if s < S and p in plan.pieces(s + 1, v, D_PIECES):
                got = z_place(s, v, p)[1]
                arrived(("z", s, v, p), got, zway[v])
                total = total + got[...].astype(F32)
        if s == 0:
            r, c = z_part(0, p)
            out[r, c] = total.astype(BF16)
            return
        src, dst = z_place(s - 1, way, p)
        src[...] = total.astype(src.dtype)
        send(("z", s - 1, way, p), src, dst, zway[way])

    run = {"A": op_a, "M": op_m, "R": op_r, "S": op_s, "F": op_f, "N": op_n, "Z": op_z}
    for (name, *at), _ in plan.schedule():
        if name == "Z" and at[0] == 0:
            for m in started[: -2 * D_PIECES]:
                m.wait_send()
            del started[: -2 * D_PIECES]
        run[name](*at)
    for m in started:
        m.wait_send()


def messages(plan):
    S = plan.S
    rings = 2 * ((S - 1) * (A_PIECES + D_PIECES) + (A_PIECES + D_PIECES) // 2)
    return rings + 2 + 2 * S * 9


def body(tokens, gate_weight, up_weight, down_weight):
    block, deep = tokens.shape
    width, cols = down_weight.shape
    chips = lax.axis_size("grid") // 2
    plan = Plan(chips, block)
    total, quarters = plan.total, plan.total // 4
    vmem, any_ = pl.BlockSpec(memory_space=pltpu.VMEM), pl.BlockSpec(memory_space=pl.ANY)
    n = messages(plan)
    return pl.pallas_call(
        functools.partial(kernel, plan),
        out_shape=pltpu.VMEM((block, cols), BF16),
        in_specs=[any_] * 4,
        out_specs=vmem,
        scratch_shapes=[
            pltpu.VMEM((total, deep), BF16),
            pltpu.VMEM((2, deep, 2 * width), BF16),
            pltpu.VMEM((2, width, cols), BF16),
            pltpu.VMEM((2 * width, deep), BF16),
            pltpu.VMEM((2, total, 2 * width), F32),
            pltpu.VMEM((2, quarters, 2 * width), BF16),
            pltpu.VMEM((2, quarters, 2 * width), BF16),
            pltpu.VMEM((2, 2, quarters, 2 * width), BF16),
            pltpu.VMEM((2, 2, quarters, 2 * width), BF16),
            pltpu.VMEM((total, 2 * width), BF16),
            pltpu.VMEM((total, cols), F32),
            pltpu.VMEM((2, total // 2, cols), BF16),
            pltpu.VMEM((2, total // 2, cols), BF16),
            pltpu.VMEM((2, max(1, WIDE_HOPS) * block, cols), F32),
            pltpu.VMEM((2, max(1, WIDE_HOPS) * block, cols), F32),
            pltpu.SemaphoreType.DMA((4,)),
            pltpu.SemaphoreType.DMA((n,)),
            pltpu.SemaphoreType.DMA((n,)),
        ],
        compiler_params=pltpu.CompilerParams(
            collective_id=0, has_side_effects=True, vmem_limit_bytes=60 * 1024 * 1024),
    )(tokens, gate_weight.T, up_weight.T, down_weight)


def solution(mesh):
    return jax.shard_map(
        body,
        mesh=mesh,
        in_specs=(P(("groups", "grid"), "depth"), P("depth", "grid"), P("depth", "grid"), P("grid", "depth")),
        out_specs=P(("groups", "grid"), "depth"),
        check_vma=False,
    )
```
